32 devices in a mesh: fsdp: 32 (over z, y, x, core).
Axes of the slice: x: 2, y: 2, z: 4, core: 2. Of those that a mesh axis runs over, the one named last changes fastest.
Arguments:
- block_input: float32 [8192, 2048], P('fsdp'), may hold values from -40 to 40
- cotangent: float32 [8192, 2048], P('fsdp'), may hold values from -6 to 6
- query_weight: bfloat16 [2048, 4096], P('fsdp'), may hold values from -0.125 to 0.125
- key_weight: bfloat16 [2048, 512], P('fsdp'), may hold values from -0.125 to 0.125
- value_weight: bfloat16 [2048, 512], P('fsdp'), may hold values from -0.125 to 0.125
- output_weight: bfloat16 [4096, 2048], P('fsdp'), may hold values from -0.375 to 0.375
- router_weight: bfloat16 [2048, 32], P('fsdp'), may hold values from -0.019897461 to 0.019897461
- norm_gains: bfloat16 [4352], P('fsdp'), may hold values from 0.25 to 1.75
- expert_gate: bfloat16 [32, 2048, 768], P('fsdp'), may hold values from -0.125 to 0.125
- expert_up: bfloat16 [32, 2048, 768], P('fsdp'), may hold values from -0.125 to 0.125
- expert_down: bfloat16 [32, 768, 2048], P('fsdp'), may hold values from -0.875 to 0.875
- routes: int32 [8192, 8], P('fsdp'), may hold values from 0 to 31, all different within a row; in each aligned block of 256 rows (0 to 255, 256 to 511, ...) at most 80 rows name the same one
- lengths: int32 [32, 4], replicated, may hold values from 1 to 128, 256 in all within a row
- assignment: int32 [32], replicated, may hold values from 0 to 31, each once
Outputs:
- block_output: float32 [8192, 2048], P('fsdp')
- input_grad: float32 [8192, 2048], P('fsdp')
- query_grad: float32 [2048, 4096], P('fsdp')
- key_grad: float32 [2048, 512], P('fsdp')
- value_grad: float32 [2048, 512], P('fsdp')
- output_grad: float32 [4096, 2048], P('fsdp')
- router_grad: float32 [2048, 32], P('fsdp')
- gains_grad: float32 [4352], P('fsdp')
- gate_grad: float32 [32, 2048, 768], P('fsdp')
- up_grad: float32 [32, 2048, 768], P('fsdp')
- down_grad: float32 [32, 768, 2048], P('fsdp')
The draws below stay inside these ranges and needn't reach their ends.
Inputs may be any that keep to these rules, and one draw needn't show every extreme that they name: `routes`: the 8 experts of a row differ; among the rows of one device no expert is named more than 80 times, a bound that some block reaches. The 4 lengths of a pack sum to 256, and the longest of each pack is 128. `assignment`: each pack is named once.
All inputs are finite; a program needn't handle non-finite values.
Results may differ from the reference program's by a relative error of at most 0.017.
Values may be sent and summed in bfloat16 or wider, within the bound.
A program may use at most 448 MiB of HBM per device.

```python
import math
import jax
import jax.numpy as jnp
import numpy as np
from jax import lax

D = 2048
H = 32
KVH = 4
HD = 128
FF = 768
TOP = 8
TOK_DEV = 256
SEQ_DEV = 4
MAXLEN = 128
EXPERTS = 32
CAP = 80
TOKENS = 8192
PACKS = 32
N_FSDP = 32


def draw_block_input(key, part):
    base_key, row_key, col_key = jax.random.split(key, 3)
    base = jnp.clip(jax.random.normal(base_key, (TOKENS, D), jnp.float32), -5.0, 5.0)
    row_scale = jnp.exp(jax.random.uniform(row_key, (TOKENS, 1), jnp.float32, math.log(0.3), math.log(3.0)))
    col_scale = jnp.exp(jax.random.uniform(col_key, (1, D), jnp.float32, -0.8, 0.8))
    return jnp.clip(base * row_scale * col_scale, -40.0, 40.0)


def levels(stream_key, shape, cuts, least, high):
    gain, own = 1.0, jax.random.fold_in(stream_key, 6)
    for dim, parts in cuts:
        draws = jnp.exp(jax.random.uniform(jax.random.fold_in(own, dim), (parts,), jnp.float32, least / len(cuts), high / len(cuts)))
        gain = gain * jnp.repeat(draws, shape[dim] // parts).reshape([-1 if axis == dim else 1 for axis in range(len(shape))])
    return gain


def length_profile(count, total, limit, slope):
    weights = [(1 << 20) // math.isqrt(standing ** slope) + 1 for standing in range(2, count + 1)]
    spare, holding = total - limit - (count - 1), [1] * (count - 1)
    while spare > 0:
        movable = [i for i in range(count - 1) if holding[i] < limit]
        mass, budget = sum([weights[i] for i in movable]), spare
        for i in movable:
            extra = min(limit - holding[i], max(1, budget * weights[i] // mass), spare)
            holding[i] = holding[i] + extra
            spare = spare - extra
    return np.array([limit] + holding)


def uneven(stream_key, count, total, reach, slope):
    if count == 2:
        one = jax.random.randint(stream_key, (), max(1, total - reach), min(reach, total - 1) + 1)
        return jnp.stack([one, total - one])
    tallies = jnp.asarray(length_profile(count, total, reach, slope), jnp.int32)
    pairs = (count - 1) // 2
    giver, receiver = tallies[1:1 + 2 * pairs:2], tallies[2:2 + 2 * pairs:2]
    slack = jnp.minimum(giver - 1, reach - receiver)
    moved = jax.random.randint(jax.random.fold_in(stream_key, 1), (pairs,), 0, 1 << 20) % (slack + 1)
    tallies = tallies.at[1:1 + 2 * pairs:2].set(giver - moved).at[2:2 + 2 * pairs:2].set(receiver + moved)
    return tallies[jax.random.permutation(jax.random.fold_in(stream_key, 2), count)]


def routed_block(own_key, own, number, rows, count, top, reach, lean):
    order = jax.random.permutation(own_key, count)
    crowded, ordinary = shares(count, rows * top, reach, lean, True), shares(count, rows * top, reach, lean, False)
    places = jnp.arange(count)

    def named(sizes, offset_by):
        used = int((sizes > 0).sum())
        fixed = max(1, used // 4)
        moved = fixed + (places - fixed + offset_by * (used - fixed)) % max(1, count - fixed)
        return jnp.zeros((count,), jnp.int32).at[order[jnp.where(places < fixed, places, moved)]].set(jnp.asarray(sizes, jnp.int32))

    sizes = jnp.where(number % 4 == 0, named(crowded, number // 4), named(ordinary, number - number // 4 - 1))
    mixed = jax.random.permutation(jax.random.fold_in(own, 3), count)
    source_of, sink = mixed[0:count // 2 * 2:2], mixed[1:count // 2 * 2:2]
    slack = jnp.minimum(sizes[source_of] - 1, reach - sizes[sink]) // 2
    slack = jnp.where((source_of == order[0]) | (sink == order[0]) | (sizes[sink] == 0), 0, jnp.maximum(slack, 0))
    moved = jax.random.randint(jax.random.fold_in(own, 4), (count // 2,), 0, 1 << 20) % (slack + 1)
    sizes = sizes.at[source_of].add(-moved).at[sink].add(moved)
    labels = jnp.searchsorted(jnp.cumsum(sizes), jnp.arange(rows * top), side="right").astype(jnp.int32)
    grid = labels.reshape(top, rows).T
    grid = grid[jax.random.permutation(jax.random.fold_in(own, 1), rows)]
    offset_by = jax.random.randint(jax.random.fold_in(own, 2), (rows, 1), 0, top)
    return jnp.take_along_axis(grid, (jnp.arange(top)[None, :] + offset_by) % top, axis=1)


def shares(amount, total, bound, slope, full):
    loads = [(1 << 20) // math.isqrt(standing ** slope) + 1 for standing in range(1, amount + 1)]
    largest = bound if full else min(bound, max(-(-total // amount), total * loads[0] // sum(loads)))
    least = 1 if total - largest >= amount - 1 else 0
    given, spare = [largest] + [least] * (amount - 1), total - largest - least * (amount - 1)
    while spare > 0:
        candidates = [i for i in range(1, amount) if given[i] < largest] or [i for i in range(1, amount) if given[i] < bound]
        whole, budget = sum([loads[i] for i in candidates]), spare
        for i in candidates:
            extra = min(bound - given[i], max(1, budget * loads[i] // whole), spare)
            given[i] = given[i] + extra
            spare = spare - extra
    return np.array(given)


def normal_values(key, extent, width, most, pieces=(), kind=jnp.bfloat16):
    level = levels(key, extent, pieces, -0.22, 0.18) if pieces else 1.0
    array = jax.random.normal(key, extent, jnp.float32) * width * level
    return jnp.minimum(jnp.maximum(array, -most), most).astype(kind)


def setup_inputs(seed: int = 0) -> dict:
    key_of = jax.random.split(jax.random.key(seed), 15)
    block_input = draw_block_input(jax.random.fold_in(key_of[14], 71), 0)
    cotangent = normal_values(key_of[1], (TOKENS, D), 1.0, 6.0, ((0, 32),), jnp.float32)
    query_weight = normal_values(key_of[2], (D, H * HD), D ** -0.5, 0.125, ((0, 32),))
    key_weight = normal_values(key_of[3], (D, KVH * HD), D ** -0.5, 0.125, ((0, 32),))
    value_weight = normal_values(key_of[4], (D, KVH * HD), D ** -0.5, 0.125, ((0, 32),))
    output_weight = normal_values(key_of[5], (H * HD, D), (H * HD // 16) ** -0.5, 0.375, ((0, 32),))
    router_weight = jnp.clip(jax.random.uniform(key_of[6], (D, EXPERTS), jnp.float32, -0.019897461, 0.019897461) * levels(key_of[6], (D, EXPERTS), ((0, 32),), -0.4, 0.0), -0.019897461, 0.019897461).astype(jnp.bfloat16)
    norm_gains = jnp.clip(1.0 + 0.15 * jax.random.normal(key_of[7], (2 * D + 2 * HD,), jnp.float32), 0.25, 1.75).astype(jnp.bfloat16)
    expert_gate = normal_values(key_of[8], (EXPERTS, D, FF), D ** -0.5, 0.125, ((0, 32),))
    expert_up = normal_values(key_of[9], (EXPERTS, D, FF), D ** -0.5, 0.125, ((0, 32),))
    expert_down = normal_values(key_of[10], (EXPERTS, FF, D), (FF // 16) ** -0.5, 0.875, ((0, 32),))
    routes_keys = jax.random.split(jax.random.fold_in(key_of[11], 1), TOKENS // TOK_DEV)
    routes_turns = jax.random.permutation(jax.random.fold_in(key_of[11], 3), TOKENS // TOK_DEV)
    routes = jax.vmap(lambda own, number: routed_block(jax.random.fold_in(key_of[11], 2), own, number, TOK_DEV, EXPERTS, TOP, CAP, 2))(routes_keys, routes_turns).reshape((TOKENS, TOP))
    lengths = jax.vmap(lambda own: uneven(own, SEQ_DEV, TOK_DEV, MAXLEN, 2))(jax.random.split(key_of[12], PACKS)).reshape((PACKS, SEQ_DEV)).astype(jnp.int32)
    assignment = jax.random.permutation(key_of[13], PACKS).astype(jnp.int32)
    return dict(block_input=block_input, cotangent=cotangent, query_weight=query_weight, key_weight=key_weight, value_weight=value_weight, output_weight=output_weight, router_weight=router_weight, norm_gains=norm_gains, expert_gate=expert_gate, expert_up=expert_up, expert_down=expert_down, routes=routes, lengths=lengths, assignment=assignment)


NORM_EPSILON = 1e-06
ROPE_BASE = 1000000.0

def rms_forward(source, scales):
    factor = lax.rsqrt(lax.optimization_barrier(jnp.mean(source * source, axis=-1, keepdims=True)) + NORM_EPSILON)
    return (source * factor * scales, factor)

def rms_backward(source, factor, scales, upstream):
    scaled = upstream * scales
    inner_mean = lax.optimization_barrier(jnp.mean(scaled * source, axis=-1, keepdims=True))
    grad_source = factor * (scaled - source * factor * factor * inner_mean)
    leading = tuple(range(source.ndim - 1))
    grad_scales = lax.optimization_barrier(jnp.sum(upstream * source * factor, axis=leading))
    return (grad_source, grad_scales)

def segment_layout(lengths_row, tokens_here):
    seq_ends = jnp.cumsum(lengths_row).astype(jnp.int32)
    places = jnp.arange(tokens_here, dtype=jnp.int32)
    passed = (places[:, None] >= seq_ends[None, :]).astype(jnp.int32)
    segment = lax.optimization_barrier(jnp.sum(passed, axis=1)).astype(jnp.int32)
    seq_start = lax.optimization_barrier(jnp.sum(passed * lengths_row[None, :], axis=1)).astype(jnp.int32)
    return (segment, places - seq_start)

def rotation_tables(offset, head_size):
    half_size = head_size // 2
    frequency = ROPE_BASE ** (-2.0 * jnp.arange(half_size, dtype=jnp.float32) / head_size)
    angles = offset.astype(jnp.float32)[:, None] * frequency[None, :]
    return (jnp.cos(angles)[:, None, :], jnp.sin(angles)[:, None, :])

def rotate(operand, cosine_table, sine_table):
    half_size = operand.shape[-1] // 2
    first_half = operand[..., :half_size]
    second_half = operand[..., half_size:]
    return jnp.concatenate([first_half * cosine_table - second_half * sine_table, second_half * cosine_table + first_half * sine_table], axis=-1)

def rotate_back(operand, cosine_table, sine_table):
    half_size = operand.shape[-1] // 2
    first_half = operand[..., :half_size]
    second_half = operand[..., half_size:]
    return jnp.concatenate([first_half * cosine_table + second_half * sine_table, second_half * cosine_table - first_half * sine_table], axis=-1)

def silu_parts(pre_act):
    logistic = jax.nn.sigmoid(pre_act)
    return (pre_act * logistic, logistic * (1.0 + pre_act * (1.0 - logistic)))

def batched(form, left, right):
    return jnp.einsum(form, left.astype(jnp.float32), right.astype(jnp.float32))

def times_transpose(left, right):
    return jnp.dot(left, right.T, preferred_element_type=jnp.float32)

def transpose_times(left, right):
    return jnp.dot(left.T, right, preferred_element_type=jnp.float32)

def split_gains(gains_vec, model_width):
    gains_float = gains_vec.astype(jnp.float32)
    return (gains_float[:model_width], gains_float[model_width:2 * model_width], gains_float[2 * model_width:2 * model_width + HD], gains_float[2 * model_width + HD:])

def attention_weights(query_grouped, key_rot, allowed, scale, totals):
    scores = batched('tkgd,ukd->kgtu', query_grouped, key_rot) * scale
    raised = jnp.where(allowed, jnp.exp(scores), 0.0)
    if totals is None:
        totals = lax.optimization_barrier(jnp.sum(raised, axis=-1, keepdims=True))
    return (raised / totals, totals)

def route_mask(routes_here, n_experts):
    return routes_here[:, :, None] == jnp.arange(n_experts, dtype=jnp.int32)[None, None, :]

def slot_tables(picked_mask, routes_here, route_weights, capacity):
    tokens_here, top_count, n_experts = picked_mask.shape
    flat_mask = picked_mask.reshape(tokens_here * top_count, n_experts).astype(jnp.int32)
    running = jnp.cumsum(flat_mask, axis=0).astype(jnp.int32)
    slot_rank = lax.optimization_barrier(jnp.sum(flat_mask * running, axis=1)).astype(jnp.int32) - 1
    slot_index = (routes_here.reshape(-1) * capacity + slot_rank).astype(jnp.int32)
    owner_row = (jnp.arange(tokens_here * top_count, dtype=jnp.int32) // top_count).astype(jnp.int32)
    slot_token = jnp.zeros((n_experts * capacity,), jnp.int32).at[slot_index].set(owner_row)
    slot_weight = jnp.zeros((n_experts * capacity,), jnp.float32).at[slot_index].set(route_weights.reshape(-1))
    slot_live = jnp.zeros((n_experts * capacity,), jnp.int32).at[slot_index].set(1)
    return (slot_index, slot_token, slot_weight, slot_live)

def dense_forward(block_rows, lengths_row, routes_here, weights_all, gains_all, n_experts):
    query_weight, key_weight, value_weight, output_weight, router_weight = weights_all
    gain_first, gain_second, gain_query, gain_key = gains_all
    tokens_here = block_rows.shape[0]
    group_size = H // KVH
    scale = HD ** (-0.5)
    segment, offset = segment_layout(lengths_row, tokens_here)
    places = jnp.arange(tokens_here, dtype=jnp.int32)
    allowed = (segment[:, None] == segment[None, :]) & (places[None, :] <= places[:, None])
    cosine_table, sine_table = rotation_tables(offset, HD)
    normed_first, factor_first = rms_forward(block_rows, gain_first)
    first_normed = normed_first.astype(jnp.bfloat16)
    query_raw = jnp.dot(first_normed, query_weight, preferred_element_type=jnp.float32).reshape(tokens_here, H, HD)
    key_raw = jnp.dot(first_normed, key_weight, preferred_element_type=jnp.float32).reshape(tokens_here, KVH, HD)
    value_rows = jnp.dot(first_normed, value_weight, preferred_element_type=jnp.float32).astype(jnp.bfloat16).reshape(tokens_here, KVH, HD)
    query_normed, query_factor = rms_forward(query_raw, gain_query)
    key_normed, key_factor = rms_forward(key_raw, gain_key)
    query_rot = rotate(query_normed, cosine_table, sine_table).astype(jnp.bfloat16)
    key_rot = rotate(key_normed, cosine_table, sine_table).astype(jnp.bfloat16)
    query_grouped = query_rot.reshape(tokens_here, KVH, group_size, HD)
    attention, totals = attention_weights(query_grouped, key_rot, allowed, scale, None)
    attention_b = attention.astype(jnp.bfloat16)
    mixed = batched('kgtu,ukd->tkgd', attention_b, value_rows).astype(jnp.bfloat16).reshape(tokens_here, H * HD)
    residual = block_rows + jnp.dot(mixed, output_weight, preferred_element_type=jnp.float32)
    normed_second, factor_second = rms_forward(residual, gain_second)
    second_normed = normed_second.astype(jnp.bfloat16)
    logits = jnp.dot(second_normed, router_weight, preferred_element_type=jnp.float32)
    picked_mask = route_mask(routes_here, n_experts)
    chosen = lax.optimization_barrier(jnp.sum(jnp.where(picked_mask, logits[:, None, :], 0.0), axis=-1))
    raised = jnp.exp(chosen)
    route_weights = raised / lax.optimization_barrier(jnp.sum(raised, axis=-1, keepdims=True))
    return {'block_rows': block_rows, 'first_normed': first_normed, 'factor_first': factor_first, 'query_raw': query_raw, 'query_factor': query_factor, 'key_raw': key_raw, 'key_factor': key_factor, 'query_grouped': query_grouped, 'key_rot': key_rot, 'value_rows': value_rows, 'allowed': allowed, 'cosine_table': cosine_table, 'sine_table': sine_table, 'totals': totals, 'mixed': mixed, 'residual': residual, 'factor_second': factor_second, 'second_normed': second_normed, 'picked_mask': picked_mask, 'route_weights': route_weights}

def dense_backward(saved, weights_all, gains_all, cotangent_rows, moe_back, route_agree):
    query_weight, key_weight, value_weight, output_weight, router_weight = weights_all
    gain_first, gain_second, gain_query, gain_key = gains_all
    tokens_here = cotangent_rows.shape[0]
    group_size = H // KVH
    scale = HD ** (-0.5)
    route_weights = saved['route_weights']
    chosen_grad = route_weights * (route_agree - lax.optimization_barrier(jnp.sum(route_weights * route_agree, axis=-1, keepdims=True)))
    logit_grad = lax.optimization_barrier(jnp.sum(jnp.where(saved['picked_mask'], chosen_grad[:, :, None], 0.0), axis=1)).astype(jnp.bfloat16)
    second_grad = moe_back + times_transpose(logit_grad, router_weight)
    router_grad = transpose_times(saved['second_normed'], logit_grad)
    residual_norm_grad, gain_second_grad = rms_backward(saved['residual'], saved['factor_second'], gain_second, second_grad)
    residual_grad = cotangent_rows + residual_norm_grad
    residual_grad_b = residual_grad.astype(jnp.bfloat16)
    output_grad = transpose_times(saved['mixed'], residual_grad_b)
    mixed_grad = times_transpose(residual_grad_b, output_weight).astype(jnp.bfloat16)
    mixed_grouped = mixed_grad.reshape(tokens_here, KVH, group_size, HD)
    attention, _ = attention_weights(saved['query_grouped'], saved['key_rot'], saved['allowed'], scale, saved['totals'])
    attention_b = attention.astype(jnp.bfloat16)
    score_grad_raw = batched('tkgd,ukd->kgtu', mixed_grouped, saved['value_rows'])
    value_rows_grad = batched('kgtu,tkgd->ukd', attention_b, mixed_grouped)
    delta = lax.optimization_barrier(jnp.sum(attention * score_grad_raw, axis=-1, keepdims=True))
    score_grad = (attention * (score_grad_raw - delta) * scale).astype(jnp.bfloat16)
    query_rot_grad = batched('kgtu,ukd->tkgd', score_grad, saved['key_rot']).reshape(tokens_here, H, HD)
    key_rot_grad = batched('kgtu,tkgd->ukd', score_grad, saved['query_grouped'])
    query_raw_grad, gain_query_grad = rms_backward(saved['query_raw'], saved['query_factor'], gain_query, rotate_back(query_rot_grad, saved['cosine_table'], saved['sine_table']))
    key_raw_grad, gain_key_grad = rms_backward(saved['key_raw'], saved['key_factor'], gain_key, rotate_back(key_rot_grad, saved['cosine_table'], saved['sine_table']))
    query_grad_b = query_raw_grad.reshape(tokens_here, H * HD).astype(jnp.bfloat16)
    key_grad_b = key_raw_grad.reshape(tokens_here, KVH * HD).astype(jnp.bfloat16)
    value_grad_b = value_rows_grad.reshape(tokens_here, KVH * HD).astype(jnp.bfloat16)
    first_grad = times_transpose(query_grad_b, query_weight) + times_transpose(key_grad_b, key_weight) + times_transpose(value_grad_b, value_weight)
    first_normed = saved['first_normed']
    query_grad = transpose_times(first_normed, query_grad_b)
    key_grad = transpose_times(first_normed, key_grad_b)
    value_grad = transpose_times(first_normed, value_grad_b)
    input_norm_grad, gain_first_grad = rms_backward(saved['block_rows'], saved['factor_first'], gain_first, first_grad)
    input_grad = residual_grad + input_norm_grad
    gains_grad = jnp.concatenate([gain_first_grad, gain_second_grad, gain_query_grad, gain_key_grad])
    return (input_grad, (query_grad, key_grad, value_grad, output_grad, router_grad, gains_grad))

def expert_forward_local(rows_in, gate_local, up_local, down_local):
    pre_gate = jnp.dot(rows_in, gate_local, preferred_element_type=jnp.float32)
    pre_up = jnp.dot(rows_in, up_local, preferred_element_type=jnp.float32)
    activated, _ = silu_parts(pre_gate)
    inner = (activated * pre_up).astype(jnp.bfloat16)
    result = jnp.dot(inner, down_local, preferred_element_type=jnp.float32).astype(jnp.bfloat16)
    return (result, pre_gate, pre_up, inner)

def expert_backward(rows_in, pre_gate, pre_up, inner, grad_rows, gate_local, up_local, down_local):
    inner_grad = times_transpose(grad_rows, down_local)
    down_grad = transpose_times(inner, grad_rows)
    activated, derivative = silu_parts(pre_gate)
    gate_pre_grad = (inner_grad * pre_up * derivative).astype(jnp.bfloat16)
    up_pre_grad = (inner_grad * activated).astype(jnp.bfloat16)
    rows_grad = (times_transpose(gate_pre_grad, gate_local) + times_transpose(up_pre_grad, up_local)).astype(jnp.bfloat16)
    return (rows_grad, transpose_times(rows_in, gate_pre_grad), transpose_times(rows_in, up_pre_grad), down_grad)

def reference(block_input, cotangent, query_weight, key_weight, value_weight, output_weight, router_weight, norm_gains, expert_gate, expert_up, expert_down, routes, lengths, assignment):
    device_count = N_FSDP
    weights_all = (query_weight, key_weight, value_weight, output_weight, router_weight)
    gains_all = split_gains(norm_gains, D)
    input_blocks = block_input.reshape(device_count, TOK_DEV, D)
    cot_blocks = cotangent.reshape(device_count, TOK_DEV, D)
    route_blocks = routes.reshape(device_count, TOK_DEV, TOP)
    pack_rows = jnp.take(lengths, assignment, axis=0)

    def forward_step(carry, inputs):
        block_rows, lengths_row, routes_here = inputs
        saved = dense_forward(block_rows, lengths_row, routes_here, weights_all, gains_all, EXPERTS)
        slot_index, slot_token, slot_weight, slot_live = slot_tables(saved['picked_mask'], routes_here, saved['route_weights'], CAP)
        return (carry, (saved['second_normed'], slot_token, slot_weight, slot_live))
    _, (normed_all, token_all, weight_all, live_all) = lax.scan(forward_step, (), (input_blocks, pack_rows, route_blocks))
    normed_flat = normed_all.reshape(TOKENS, D)
    base_rows = (jnp.arange(device_count, dtype=jnp.int32) * TOK_DEV)[:, None, None]
    token_global = (token_all.reshape(device_count, EXPERTS, CAP) + base_rows).astype(jnp.int32)
    token_global = token_global.transpose(1, 0, 2).reshape(EXPERTS, device_count * CAP)
    weight_global = weight_all.reshape(device_count, EXPERTS, CAP).transpose(1, 0, 2).reshape(EXPERTS, device_count * CAP)
    live_global = live_all.reshape(device_count, EXPERTS, CAP).transpose(1, 0, 2).reshape(EXPERTS, device_count * CAP)

    def expert_step(carry, inputs):
        moe_sum, back_sum = carry
        gate_local, up_local, down_local, row_index, slot_weight, slot_live = inputs
        rows_in = jnp.where(slot_live[:, None] > 0, jnp.take(normed_flat, row_index, axis=0), jnp.zeros((), jnp.bfloat16))
        result, pre_gate, pre_up, inner = expert_forward_local(rows_in, gate_local, up_local, down_local)
        cot_rows = jnp.take(cotangent, row_index, axis=0)
        grad_rows = (cot_rows * slot_weight[:, None]).astype(jnp.bfloat16)
        result_float = result.astype(jnp.float32)
        agree_slot = lax.optimization_barrier(jnp.sum(cot_rows * result_float, axis=-1))
        rows_grad, gate_grad, up_grad, down_grad = expert_backward(rows_in, pre_gate, pre_up, inner, grad_rows, gate_local, up_local, down_local)
        moe_sum = moe_sum.at[row_index].add(result_float * slot_weight[:, None])
        back_sum = back_sum.at[row_index].add(rows_grad.astype(jnp.float32))
        return ((moe_sum, back_sum), (gate_grad, up_grad, down_grad, agree_slot))
    zero_rows = jnp.zeros((TOKENS, D), jnp.float32)
    (moe_sum, back_sum), (gate_grads, up_grads, down_grads, agree_all) = lax.scan(expert_step, (zero_rows, zero_rows), (expert_gate, expert_up, expert_down, token_global, weight_global, live_global))
    agree_dev = agree_all.reshape(EXPERTS, device_count, CAP).transpose(1, 0, 2).reshape(device_count, EXPERTS * CAP)
    moe_blocks = moe_sum.reshape(device_count, TOK_DEV, D)
    back_blocks = back_sum.reshape(device_count, TOK_DEV, D)

    def backward_step(carry, inputs):
        block_rows, lengths_row, routes_here, cot_rows, moe_rows, back_rows, agree_row = inputs
        saved = dense_forward(block_rows, lengths_row, routes_here, weights_all, gains_all, EXPERTS)
        slot_index, slot_token, slot_weight, slot_live = slot_tables(saved['picked_mask'], routes_here, saved['route_weights'], CAP)
        route_agree = jnp.take(agree_row, slot_index, axis=0).reshape(TOK_DEV, TOP)
        input_grad, grads = dense_backward(saved, weights_all, gains_all, cot_rows, back_rows, route_agree)
        summed = tuple((held + fresh for held, fresh in zip(carry, grads)))
        return (summed, (saved['residual'] + moe_rows, input_grad))
    zero_grads = (jnp.zeros((D, H * HD), jnp.float32), jnp.zeros((D, KVH * HD), jnp.float32), jnp.zeros((D, KVH * HD), jnp.float32), jnp.zeros((H * HD, D), jnp.float32), jnp.zeros((D, EXPERTS), jnp.float32), jnp.zeros((2 * D + 2 * HD,), jnp.float32))
    grads, (output_blocks, input_grad_blocks) = lax.scan(backward_step, zero_grads, (input_blocks, pack_rows, route_blocks, cot_blocks, moe_blocks, back_blocks, agree_dev))
    return (output_blocks.reshape(TOKENS, D), input_grad_blocks.reshape(TOKENS, D), grads[0], grads[1], grads[2], grads[3], grads[4], grads[5], gate_grads, up_grads, down_grads)
```

```python
import functools
import types

import jax
import jax.numpy as jnp
from jax import lax
from jax.experimental import pallas as pl
from jax.experimental.pallas import tpu as pltpu
from jax.sharding import PartitionSpec as P

H = 32
KVH = 4
HD = 128
TOP = 8
AXIS = "fsdp"


NORM_EPSILON = 1e-06
ROPE_BASE = 1000000.0


def rms_forward(source, scales):
    factor = lax.rsqrt(jnp.mean(source * source, axis=-1, keepdims=True) + NORM_EPSILON)
    return (source * factor * scales, factor)


def rms_backward(source, factor, scales, upstream):
    scaled = upstream * scales
    inner_mean = jnp.mean(scaled * source, axis=-1, keepdims=True)
    grad_source = factor * (scaled - source * factor * factor * inner_mean)
    leading = tuple(range(source.ndim - 1))
    grad_scales = jnp.sum(upstream * source * factor, axis=leading)
    return (grad_source, grad_scales)


def segment_layout(lengths_row, tokens_here):
    seq_ends = jnp.cumsum(lengths_row)
    places = jnp.arange(tokens_here, dtype=jnp.int32)
    passed = (places[:, None] >= seq_ends[None, :]).astype(jnp.int32)
    segment = jnp.sum(passed, axis=1)
    seq_start = jnp.sum(passed * lengths_row[None, :], axis=1)
    return (segment, places - seq_start)


def rotation_tables(offset, head_size):
    half_size = head_size // 2
    frequency = ROPE_BASE ** (-2.0 * jnp.arange(half_size, dtype=jnp.float32) / head_size)
    angles = offset.astype(jnp.float32)[:, None] * frequency[None, :]
    return (jnp.cos(angles)[:, None, :], jnp.sin(angles)[:, None, :])


def rotate(operand, cosine_table, sine_table):
    half_size = operand.shape[-1] // 2
    first_half = operand[..., :half_size]
    second_half = operand[..., half_size:]
    return jnp.concatenate(
        [
            first_half * cosine_table - second_half * sine_table,
            second_half * cosine_table + first_half * sine_table,
        ],
        axis=-1,
    )


def rotate_back(operand, cosine_table, sine_table):
    half_size = operand.shape[-1] // 2
    first_half = operand[..., :half_size]
    second_half = operand[..., half_size:]
    return jnp.concatenate(
        [
            first_half * cosine_table + second_half * sine_table,
            second_half * cosine_table - first_half * sine_table,
        ],
        axis=-1,
    )


def silu_parts(pre_act):
    logistic = jax.nn.sigmoid(pre_act)
    return (pre_act * logistic, logistic * (1.0 + pre_act * (1.0 - logistic)))


def batched(form, left, right):
    return jnp.einsum(form, left, right, preferred_element_type=jnp.float32)


def times_transpose(left, right):
    return lax.dot_general(
        left, right, (((1,), (1,)), ((), ())), preferred_element_type=jnp.float32
    )


def transpose_times(left, right):
    return lax.dot_general(
        left, right, (((0,), (0,)), ((), ())), preferred_element_type=jnp.float32
    )


def split_gains(gains_vec, model_width):
    gains_float = gains_vec.astype(jnp.float32)
    return (
        gains_float[:model_width],
        gains_float[model_width : 2 * model_width],
        gains_float[2 * model_width : 2 * model_width + HD],
        gains_float[2 * model_width + HD :],
    )


def attention_weights(query_grouped, key_rot, allowed, scale, totals):
    scores = batched("tkgd,ukd->kgtu", query_grouped, key_rot) * scale
    raised = jnp.where(allowed, jnp.exp(scores), 0.0)
    if totals is None:
        totals = jnp.sum(raised, axis=-1, keepdims=True)
    return (raised / totals, totals)


def route_mask(routes_here, n_experts):
    return routes_here[:, :, None] == jnp.arange(n_experts, dtype=jnp.int32)[None, None, :]


def slot_tables(picked_mask, routes_here, route_weights, capacity):
    tokens_here, top_count, n_experts = picked_mask.shape
    flat_mask = picked_mask.reshape(tokens_here * top_count, n_experts).astype(jnp.int32)
    running = jnp.cumsum(flat_mask, axis=0)
    slot_rank = jnp.sum(flat_mask * running, axis=1) - 1
    slot_index = routes_here.reshape(-1) * capacity + slot_rank
    owner_row = jnp.arange(tokens_here * top_count, dtype=jnp.int32) // top_count
    slot_token = jnp.zeros((n_experts * capacity,), jnp.int32).at[slot_index].set(owner_row)
    slot_weight = (
        jnp.zeros((n_experts * capacity,), jnp.float32)
        .at[slot_index]
        .set(route_weights.reshape(-1))
    )
    slot_live = jnp.zeros((n_experts * capacity,), jnp.int32).at[slot_index].set(1)
    return (slot_index, slot_token, slot_weight, slot_live)


def dense_forward(block_rows, lengths_row, routes_here, weights_all, gains_all, n_experts):
    query_weight, key_weight, value_weight, output_weight, router_weight = weights_all
    gain_first, gain_second, gain_query, gain_key = gains_all
    tokens_here = block_rows.shape[0]
    group_size = H // KVH
    scale = HD ** (-0.5)
    segment, offset = segment_layout(lengths_row, tokens_here)
    places = jnp.arange(tokens_here, dtype=jnp.int32)
    allowed = (segment[:, None] == segment[None, :]) & (places[None, :] <= places[:, None])
    cosine_table, sine_table = rotation_tables(offset, HD)
    normed_first, factor_first = rms_forward(block_rows, gain_first)
    first_normed = normed_first.astype(jnp.bfloat16)
    query_raw = jnp.dot(first_normed, query_weight, preferred_element_type=jnp.float32).reshape(
        tokens_here, H, HD
    )
    key_raw = jnp.dot(first_normed, key_weight, preferred_element_type=jnp.float32).reshape(
        tokens_here, KVH, HD
    )
    value_rows = (
        jnp.dot(first_normed, value_weight, preferred_element_type=jnp.float32)
        .astype(jnp.bfloat16)
        .reshape(tokens_here, KVH, HD)
    )
    query_normed, query_factor = rms_forward(query_raw, gain_query)
    key_normed, key_factor = rms_forward(key_raw, gain_key)
    query_rot = rotate(query_normed, cosine_table, sine_table).astype(jnp.bfloat16)
    key_rot = rotate(key_normed, cosine_table, sine_table).astype(jnp.bfloat16)
    query_grouped = query_rot.reshape(tokens_here, KVH, group_size, HD)
    attention, totals = attention_weights(query_grouped, key_rot, allowed, scale, None)
    attention_b = attention.astype(jnp.bfloat16)
    mixed = (
        batched("kgtu,ukd->tkgd", attention_b, value_rows)
        .astype(jnp.bfloat16)
        .reshape(tokens_here, H * HD)
    )
    residual = block_rows + jnp.dot(mixed, output_weight, preferred_element_type=jnp.float32)
    normed_second, factor_second = rms_forward(residual, gain_second)
    second_normed = normed_second.astype(jnp.bfloat16)
    logits = jnp.dot(second_normed, router_weight, preferred_element_type=jnp.float32)
    picked_mask = route_mask(routes_here, n_experts)
    chosen = jnp.sum(jnp.where(picked_mask, logits[:, None, :], 0.0), axis=-1)
    raised = jnp.exp(chosen)
    route_weights = raised / jnp.sum(raised, axis=-1, keepdims=True)
    return types.SimpleNamespace(
        block_rows=block_rows,
        first_normed=first_normed,
        factor_first=factor_first,
        query_raw=query_raw,
        query_factor=query_factor,
        key_raw=key_raw,
        key_factor=key_factor,
        query_grouped=query_grouped,
        key_rot=key_rot,
        value_rows=value_rows,
        allowed=allowed,
        cosine_table=cosine_table,
        sine_table=sine_table,
        totals=totals,
        mixed=mixed,
        residual=residual,
        factor_second=factor_second,
        second_normed=second_normed,
        picked_mask=picked_mask,
        route_weights=route_weights,
    )


def sparse_backward(saved, weights_all, gains_all, cotangent_rows, moe_back, route_agree):
    query_weight, key_weight, value_weight, output_weight, router_weight = weights_all
    gain_first, gain_second, gain_query, gain_key = gains_all
    tokens_here = cotangent_rows.shape[0]
    group_size = H // KVH
    scale = HD ** (-0.5)
    route_weights = saved.route_weights
    chosen_grad = route_weights * (
        route_agree - jnp.sum(route_weights * route_agree, axis=-1, keepdims=True)
    )
    logit_grad = jnp.sum(
        jnp.where(saved.picked_mask, chosen_grad[:, :, None], 0.0), axis=1
    ).astype(jnp.bfloat16)
    second_grad = moe_back + times_transpose(logit_grad, router_weight)
    router_grad = transpose_times(saved.second_normed, logit_grad)
    residual_norm_grad, gain_second_grad = rms_backward(
        saved.residual, saved.factor_second, gain_second, second_grad
    )
    residual_grad = cotangent_rows + residual_norm_grad
    residual_grad_b = residual_grad.astype(jnp.bfloat16)
    output_grad = transpose_times(saved.mixed, residual_grad_b)
    mixed_grad = times_transpose(residual_grad_b, output_weight).astype(jnp.bfloat16)
    mixed_grouped = mixed_grad.reshape(tokens_here, KVH, group_size, HD)
    attention, _ = attention_weights(
        saved.query_grouped, saved.key_rot, saved.allowed, scale, saved.totals
    )
    attention_b = attention.astype(jnp.bfloat16)
    score_grad_raw = batched("tkgd,ukd->kgtu", mixed_grouped, saved.value_rows)
    value_rows_grad = batched("kgtu,tkgd->ukd", attention_b, mixed_grouped)
    delta = jnp.sum(attention * score_grad_raw, axis=-1, keepdims=True)
    score_grad = (attention * (score_grad_raw - delta) * scale).astype(jnp.bfloat16)
    query_rot_grad = batched("kgtu,ukd->tkgd", score_grad, saved.key_rot).reshape(
        tokens_here, H, HD
    )
    key_rot_grad = batched("kgtu,tkgd->ukd", score_grad, saved.query_grouped)
    query_raw_grad, gain_query_grad = rms_backward(
        saved.query_raw,
        saved.query_factor,
        gain_query,
        rotate_back(query_rot_grad, saved.cosine_table, saved.sine_table),
    )
    key_raw_grad, gain_key_grad = rms_backward(
        saved.key_raw,
        saved.key_factor,
        gain_key,
        rotate_back(key_rot_grad, saved.cosine_table, saved.sine_table),
    )
    query_grad_b = query_raw_grad.reshape(tokens_here, H * HD).astype(jnp.bfloat16)
    key_grad_b = key_raw_grad.reshape(tokens_here, KVH * HD).astype(jnp.bfloat16)
    value_grad_b = value_rows_grad.reshape(tokens_here, KVH * HD).astype(jnp.bfloat16)
    first_grad = (
        times_transpose(query_grad_b, query_weight)
        + times_transpose(key_grad_b, key_weight)
        + times_transpose(value_grad_b, value_weight)
    )
    first_normed = saved.first_normed
    query_grad = transpose_times(first_normed, query_grad_b)
    key_grad = transpose_times(first_normed, key_grad_b)
    value_grad = transpose_times(first_normed, value_grad_b)
    input_norm_grad, gain_first_grad = rms_backward(
        saved.block_rows, saved.factor_first, gain_first, first_grad
    )
    input_grad = residual_grad + input_norm_grad
    gains_grad = jnp.concatenate(
        [gain_first_grad, gain_second_grad, gain_query_grad, gain_key_grad]
    )
    return (input_grad, (query_grad, key_grad, value_grad, output_grad, router_grad, gains_grad))


def expert_forward_local(rows_in, gate_local, up_local, down_local):
    pre_gate = jnp.dot(rows_in, gate_local, preferred_element_type=jnp.float32)
    pre_up = jnp.dot(rows_in, up_local, preferred_element_type=jnp.float32)
    activated, _ = silu_parts(pre_gate)
    inner = (activated * pre_up).astype(jnp.bfloat16)
    result = jnp.dot(inner, down_local, preferred_element_type=jnp.float32).astype(jnp.bfloat16)
    return (result, pre_gate, pre_up, inner)


def expert_backward(rows_in, pre_gate, pre_up, inner, grad_rows, gate_local, up_local, down_local):
    inner_grad = times_transpose(grad_rows, down_local)
    down_grad = transpose_times(inner, grad_rows)
    activated, derivative = silu_parts(pre_gate)
    gate_pre_grad = (inner_grad * pre_up * derivative).astype(jnp.bfloat16)
    up_pre_grad = (inner_grad * activated).astype(jnp.bfloat16)
    rows_grad = (
        times_transpose(gate_pre_grad, gate_local) + times_transpose(up_pre_grad, up_local)
    ).astype(jnp.bfloat16)
    return (
        rows_grad,
        transpose_times(rows_in, gate_pre_grad),
        transpose_times(rows_in, up_pre_grad),
        down_grad,
    )


def swap(value, n_devices, mask):
    return lax.ppermute(value, AXIS, [(i, i ^ mask) for i in range(n_devices)])


def hop(value, n_devices, even_mask, odd_mask):
    pairs = [(i, i ^ (odd_mask if i & 1 else even_mask)) for i in range(n_devices)]
    return lax.ppermute(value, AXIS, pairs)


def first_hop(value, n_devices):
    return hop(value, n_devices, 2, 4)


def second_hop(value, n_devices):
    return hop(value, n_devices, 4, 2)


def block_sources(device, n_devices):
    core = device & 1
    one = 2 + 2 * core
    offsets = [jnp.zeros_like(device), one, 6 - one, jnp.full_like(device, 6)]
    return jnp.stack([device ^ off ^ (8 * g) for g in range(n_devices // 8) for off in offsets])


def collect(make, n_devices, dtype=jnp.bfloat16):
    arrived = []
    total = None
    for g in reversed(range(n_devices // 8)):
        three = second_hop(make(4 * g + 3).astype(dtype), n_devices)
        two = second_hop(make(4 * g + 2).astype(dtype), n_devices)
        side = (make(4 * g + 1) + three.astype(jnp.float32)).astype(dtype)
        one = first_hop(side, n_devices)
        held = make(4 * g) + two.astype(jnp.float32) + one.astype(jnp.float32)
        if g:
            arrived.append(swap(held.astype(dtype), n_devices, 8 * g))
        else:
            total = held
    for part in arrived:
        total = total + part.astype(jnp.float32)
    return total


def after(value, token):
    return lax.optimization_barrier((value, token))[0]


def gather_small(value, device, n_devices):
    held = value[None]
    mask = 1
    while mask < n_devices:
        held = jnp.concatenate([held, swap(held, n_devices, mask)], axis=0)
        mask *= 2
    return jnp.take(held, device ^ jnp.arange(n_devices, dtype=jnp.int32), axis=0)


def sum_small(value, n_devices):
    mask = 1
    while mask < n_devices:
        value = value + swap(value, n_devices, mask)
        mask *= 2
    return value


def exchange_small(value, device, n_devices):
    held = value[device ^ jnp.arange(n_devices, dtype=jnp.int32)][:, None]
    mask = n_devices // 2
    while mask:
        held = jnp.concatenate([held[:mask], swap(held[mask:], n_devices, mask)], axis=1)
        mask //= 2
    bits = n_devices.bit_length() - 1
    order = [int(format(m, "0%db" % bits)[::-1], 2) for m in range(n_devices)]
    held = jnp.stack([held[0, m] for m in order])
    return jnp.take(held, device ^ jnp.arange(n_devices, dtype=jnp.int32), axis=0)


def flipped(index, mask):
    return index + mask * (1 - 2 * lax.rem(lax.div(index, mask), 2))


def hop_peers(index):
    core = lax.rem(index, 2)
    low, high = flipped(index, 2), flipped(index, 4)
    return low + core * (high - low), high + core * (low - high)


def plane_peer(index, g):
    bit = 1
    while bit <= g:
        if g & bit:
            index = flipped(index, 8 * bit)
        bit *= 2
    return index


def gather_kernel(n_devices, whole, *refs):
    count = len(whole)
    blocks, outs = refs[:count], refs[count : 2 * count]
    send, recv, here = refs[2 * count :]
    groups = n_devices // 8
    me = lax.axis_index(AXIS)
    one_peer, two_peer = hop_peers(me)
    pair = flipped(me, 1)
    planes = [plane_peer(me, g) for g in range(groups)]

    barrier = pltpu.get_barrier_semaphore()
    peers = [one_peer, two_peer, pair] + planes[1:]
    for peer in peers:
        pl.semaphore_signal(
            barrier, inc=1, device_id=(peer,), device_id_type=pl.DeviceIdType.MESH
        )
    pl.semaphore_wait(barrier, len(peers))

    def source(g, j):
        first, second = hop_peers(planes[g])
        return (planes[g], first, second, flipped(flipped(planes[g], 2), 4))[j]

    def slot(a, g, j):
        if whole[a]:
            rows = blocks[a].shape[0]
            return outs[a].at[pl.ds(pl.multiple_of(source(g, j) * rows, rows), rows)]
        return outs[a].at[4 * g + j]

    def remote(a, index, start_from, target, peer):
        return pltpu.make_async_remote_copy(
            src_ref=start_from,
            dst_ref=target,
            send_sem=send.at[a, index],
            recv_sem=recv.at[a, index],
            device_id=(peer,),
            device_id_type=pl.DeviceIdType.MESH,
        )

    def piece(a, g, j):
        return blocks[a] if g == 0 and j == 0 else slot(a, g, j)

    def remote_slot(a, g, j, target_g, target_j):
        if whole[a]:
            return slot(a, g, j)
        return outs[a].at[4 * target_g + target_j]

    started = []

    def begin(copy):
        copy.start()
        started.append(copy)
        return copy

    hops = {}
    own = []
    for a in range(count):
        if whole[a]:
            keep = pltpu.make_async_copy(blocks[a], slot(a, 0, 0), here.at[a])
            keep.start()
            own.append(keep)
    for a in range(count):
        hops[a, 0, 1] = begin(remote(a, 1, blocks[a], remote_slot(a, 0, 0, 0, 1), one_peer))
        hops[a, 0, 2] = begin(remote(a, 2, blocks[a], remote_slot(a, 0, 0, 0, 2), two_peer))
        for g in range(1, groups):
            hops[a, g, 0] = begin(
                remote(a, 4 * g, blocks[a], remote_slot(a, 0, 0, g, 0), planes[g])
            )
        if whole[a]:
            begin(remote(a, 4 * groups, blocks[a], slot(a, 0, 0), pair))

    def pass_on(a, g, j):
        if whole[a]:
            begin(remote(a, 4 * groups + 4 * g + j, piece(a, g, j), slot(a, g, j), pair))

    for g in range(groups):
        if g:
            for a in range(count):
                hops[a, g, 0].wait_recv()
                here_now = slot(a, g, 0)
                hops[a, g, 1] = begin(
                    remote(a, 4 * g + 1, here_now, remote_slot(a, g, 0, g, 1), one_peer)
                )
                hops[a, g, 2] = begin(
                    remote(a, 4 * g + 2, here_now, remote_slot(a, g, 0, g, 2), two_peer)
                )
                pass_on(a, g, 0)
        for a in range(count):
            hops[a, g, 1].wait_recv()
            hops[a, g, 3] = begin(
                remote(a, 4 * g + 3, slot(a, g, 1), remote_slot(a, g, 1, g, 3), two_peer)
            )
            pass_on(a, g, 1)
        if g:
            for a in range(count):
                hops[a, g - 1, 2].wait_recv()
                pass_on(a, g - 1, 2)
                hops[a, g - 1, 3].wait_recv()
                pass_on(a, g - 1, 3)
    for a in range(count):
        hops[a, groups - 1, 2].wait_recv()
        pass_on(a, groups - 1, 2)
        hops[a, groups - 1, 3].wait_recv()
        pass_on(a, groups - 1, 3)
    for a in range(count):
        if whole[a]:
            for g in range(groups):
                for j in range(4):
                    remote(
                        a, 4 * groups + 4 * g + j, blocks[a], slot(a, 0, 0), pair
                    ).wait_recv()
    for copy in started:
        copy.wait_send()
    for keep in own:
        keep.wait()


def gather_blocks(blocks, whole, n_devices, collective_id):
    count = len(blocks)
    slots = n_devices // 2
    shapes = [
        jax.ShapeDtypeStruct(
            (n_devices * b.shape[0],) + b.shape[1:] if w else (slots,) + b.shape, b.dtype
        )
        for b, w in zip(blocks, whole)
    ]
    return pl.pallas_call(
        functools.partial(gather_kernel, n_devices, tuple(whole)),
        out_shape=shapes,
        in_specs=[pl.BlockSpec(memory_space=pltpu.VMEM)] * count,
        out_specs=[pl.BlockSpec(memory_space=pl.ANY)] * count,
        scratch_shapes=[
            pltpu.SemaphoreType.DMA((count, 2 * slots)),
            pltpu.SemaphoreType.DMA((count, 2 * slots)),
            pltpu.SemaphoreType.DMA((count,)),
        ],
        compiler_params=pltpu.CompilerParams(
            collective_id=collective_id, has_side_effects=True
        ),
    )(*blocks)


def scatter_rows(full, sources, n_devices):
    rows = full.shape[0] // n_devices
    device = lax.axis_index(AXIS)
    split = full.reshape(n_devices // 2, 2, rows, full.shape[1])
    core = device & 1
    mine = lax.dynamic_index_in_dim(split, core, axis=1, keepdims=False)
    given = lax.dynamic_index_in_dim(split, 1 - core, axis=1, keepdims=False)
    taken = swap(given.astype(jnp.bfloat16), n_devices, 1)

    def make(index):
        chip = sources[index] // 2
        own = lax.dynamic_index_in_dim(mine, chip, axis=0, keepdims=False)
        more = lax.dynamic_index_in_dim(taken, chip, axis=0, keepdims=False)
        return own + more.astype(jnp.float32)

    return collect(make, n_devices)


def slot_choice(routes_from, expert, capacity):
    member = jnp.any(routes_from == expert[:, None, None], axis=1)
    tokens_here = member.shape[1]
    places = jnp.arange(tokens_here, dtype=jnp.int32)
    upto = (places[:, None] <= places[None, :]).astype(jnp.bfloat16)
    rank = jnp.dot(member.astype(jnp.bfloat16), upto, preferred_element_type=jnp.float32) - 1.0
    slots = jnp.arange(capacity, dtype=jnp.float32)
    return member[:, None, :] & (rank[:, None, :] == slots[None, :, None])


def weight_of(routes_from, weights_from, expert):
    return jnp.sum(jnp.where(routes_from == expert[:, None, None], weights_from, 0.0), axis=1)


def gathered_slots(pieces, choice, n_devices):
    capacity = choice.shape[1] // 2
    mine, given = [], []
    for index, piece in enumerate(pieces):
        rows = jnp.dot(choice[index], piece, preferred_element_type=jnp.float32)
        rows = rows.astype(jnp.bfloat16)
        mine.append(rows[:capacity])
        given.append(rows[capacity:])
    taken = []
    for g in range(0, len(given), 4):
        taken.append(swap(jnp.concatenate(given[g : g + 4], axis=0), n_devices, 1))
    return jnp.concatenate(mine + taken, axis=0)


def returned_sum(rows, choice, n_devices):
    blocks, double, tokens_here = choice.shape
    capacity = double // 2
    half = blocks * capacity
    taken = swap(rows[half:], n_devices, 1)

    def make(index):
        own = rows[index * capacity : (index + 1) * capacity]
        more = taken[index * capacity : (index + 1) * capacity]
        return transpose_times(choice[index], jnp.concatenate([own, more], axis=0))

    return collect(make, n_devices)


def turned(value, cosines, sines):
    return value * cosines + pltpu.roll(value, value.shape[-1] // 2, 1) * sines


def turned_back(value, cosines, sines):
    return value * cosines - pltpu.roll(value, value.shape[-1] // 2, 1) * sines


def unit_factor(value):
    return lax.rsqrt(jnp.mean(value * value, axis=-1, keepdims=True) + NORM_EPSILON)


def head_weights(query, key, allowed, scale):
    raised = jnp.where(allowed, jnp.exp(times_transpose(query, key) * scale), 0.0)
    return raised * (1.0 / jnp.sum(raised, axis=-1, keepdims=True))


def attention_kernel(scale, query_ref, key_ref, value_ref, table_ref, gain_ref, allowed_ref, out_ref):
    cosines, sines = table_ref[0], table_ref[1]
    gain_query, gain_key = gain_ref[0:1], gain_ref[1:2]
    allowed = allowed_ref[...] > 0.0
    key = key_ref[...]
    key = turned(key * unit_factor(key) * gain_key, cosines, sines).astype(jnp.bfloat16)
    value = value_ref[...].astype(jnp.bfloat16)
    for head in range(query_ref.shape[1] // HD):
        lanes = slice(head * HD, (head + 1) * HD)
        query = query_ref[:, lanes]
        query = turned(query * unit_factor(query) * gain_query, cosines, sines)
        weights = head_weights(query.astype(jnp.bfloat16), key, allowed, scale)
        mixed = jnp.dot(weights.astype(jnp.bfloat16), value, preferred_element_type=jnp.float32)
        out_ref[:, lanes] = mixed.astype(jnp.bfloat16)


def norm_back(source, factor, gain, upstream):
    scaled = upstream * gain
    inner = jnp.mean(scaled * source, axis=-1, keepdims=True)
    return factor * (scaled - source * (factor * factor * inner))


def attention_back_kernel(
    scale,
    query_ref,
    key_ref,
    value_ref,
    grad_ref,
    table_ref,
    gain_ref,
    allowed_ref,
    out_ref,
    gain_out_ref,
):
    group = pl.program_id(0)
    groups = pl.num_programs(0)
    cosines, sines = table_ref[0], table_ref[1]
    gain_query, gain_key = gain_ref[0:1], gain_ref[1:2]
    allowed = allowed_ref[...] > 0.0
    width = query_ref.shape[1]

    @pl.when(group == 0)
    def _():
        gain_out_ref[...] = jnp.zeros_like(gain_out_ref)

    key_raw = key_ref[...]
    key_factor = unit_factor(key_raw)
    key = turned(key_raw * key_factor * gain_key, cosines, sines).astype(jnp.bfloat16)
    value = value_ref[...].astype(jnp.bfloat16)
    key_grad = jnp.zeros(key_raw.shape, jnp.float32)
    value_grad = jnp.zeros(key_raw.shape, jnp.float32)
    gain_sum = jnp.zeros((1, HD), jnp.float32)
    for head in range(width // HD):
        lanes = slice(head * HD, (head + 1) * HD)
        query_raw = query_ref[:, lanes]
        query_factor = unit_factor(query_raw)
        unit = query_raw * query_factor
        query = turned(unit * gain_query, cosines, sines).astype(jnp.bfloat16)
        weights = head_weights(query, key, allowed, scale)
        mixed_grad = grad_ref[:, lanes]
        raw_grad = times_transpose(mixed_grad, value)
        delta = jnp.sum(weights * raw_grad, axis=-1, keepdims=True)
        score_grad = (weights * (raw_grad - delta) * scale).astype(jnp.bfloat16)
        value_grad += transpose_times(weights.astype(jnp.bfloat16), mixed_grad)
        key_grad += transpose_times(score_grad, query)
        upstream = turned_back(
            jnp.dot(score_grad, key, preferred_element_type=jnp.float32), cosines, sines
        )
        gain_sum += jnp.sum(upstream * unit, axis=0, keepdims=True)
        query_grad = norm_back(query_raw, query_factor, gain_query, upstream)
        start = pl.multiple_of(group * width + head * HD, HD)
        out_ref[:, pl.ds(start, HD)] = query_grad.astype(jnp.bfloat16)
    upstream = turned_back(key_grad, cosines, sines)
    gain_out_ref[0:1] += gain_sum
    gain_out_ref[1:2] += jnp.sum(upstream * key_raw * key_factor, axis=0, keepdims=True)
    start = pl.multiple_of(groups * width + group * HD, HD)
    out_ref[:, pl.ds(start, HD)] = norm_back(key_raw, key_factor, gain_key, upstream).astype(
        jnp.bfloat16
    )
    start = pl.multiple_of(groups * (width + HD) + group * HD, HD)
    out_ref[:, pl.ds(start, HD)] = value_grad.astype(jnp.bfloat16)


def attention_specs(tokens_here):
    group = H // KVH
    return [
        pl.BlockSpec((tokens_here, group * HD), lambda k: (0, k)),
        pl.BlockSpec((tokens_here, HD), lambda k: (0, H + k)),
        pl.BlockSpec((tokens_here, HD), lambda k: (0, H + KVH + k)),
    ]


def shared_specs(arrays):
    return [pl.BlockSpec(a.shape, lambda k, r=a.ndim: (0,) * r) for a in arrays]


def attention_forward(raw, tables, gains, allowed):
    tokens_here = raw.shape[0]
    group = H // KVH
    return pl.pallas_call(
        functools.partial(attention_kernel, HD ** (-0.5)),
        grid=(KVH,),
        out_shape=jax.ShapeDtypeStruct((tokens_here, H * HD), jnp.bfloat16),
        in_specs=attention_specs(tokens_here) + shared_specs([tables, gains, allowed]),
        out_specs=pl.BlockSpec((tokens_here, group * HD), lambda k: (0, k)),
        cost_estimate=pl.CostEstimate(
            flops=4 * H * HD * tokens_here**2,
            bytes_accessed=6 * raw.size,
            transcendentals=H * tokens_here**2,
        ),
    )(raw, raw, raw, tables, gains, allowed)


def attention_backward(raw, mixed_grad, tables, gains, allowed):
    tokens_here = raw.shape[0]
    group = H // KVH
    specs = attention_specs(tokens_here)
    return pl.pallas_call(
        functools.partial(attention_back_kernel, HD ** (-0.5)),
        grid=(KVH,),
        out_shape=[
            jax.ShapeDtypeStruct(raw.shape, jnp.bfloat16),
            jax.ShapeDtypeStruct((8, HD), jnp.float32),
        ],
        in_specs=specs + [specs[0]] + shared_specs([tables, gains, allowed]),
        out_specs=[
            pl.BlockSpec(raw.shape, lambda k: (0, 0)),
            pl.BlockSpec((8, HD), lambda k: (0, 0)),
        ],
        cost_estimate=pl.CostEstimate(
            flops=10 * H * HD * tokens_here**2,
            bytes_accessed=8 * raw.size,
            transcendentals=H * tokens_here**2,
        ),
    )(raw, raw, raw, mixed_grad, tables, gains, allowed)


def dense_body(
    block_input,
    cotangent,
    query_weight,
    key_weight,
    value_weight,
    output_weight,
    router_weight,
    norm_gains,
    expert_gate,
    expert_up,
    expert_down,
    routes,
    lengths,
    assignment,
):
    tokens_here, model_width = block_input.shape
    n_experts = router_weight.shape[1]
    n_devices = n_experts
    capacity = tokens_here * TOP * 5 // (4 * n_experts)
    device = lax.axis_index(AXIS)
    sources = block_sources(device, n_devices)
    other_sources = block_sources(device ^ 1, n_devices)

    gain_count = norm_gains.shape[0]
    router_count = router_weight.size
    small = jnp.concatenate(
        [router_weight.reshape(-1), norm_gains, routes.T.astype(jnp.bfloat16).reshape(-1)]
    )
    padded = -(-small.shape[0] // 2048) * 2048
    small = jnp.pad(small, (0, padded - small.shape[0])).reshape(-1, 128)
    joined = jnp.concatenate([query_weight, key_weight, value_weight], axis=1)
    small_all, joined_all, output_all = gather_blocks(
        [small, joined, output_weight], [True, True, True], n_devices, 0
    )
    small_all = small_all.reshape(n_devices, -1)
    router_all = small_all[:, :router_count].reshape(-1, n_experts)
    route_start = router_count + gain_count
    gains_all = split_gains(small_all[:, router_count:route_start].reshape(-1), model_width)
    routes_all = small_all[:, route_start : route_start + routes.size]
    routes_all = routes_all.reshape(n_devices, TOP, tokens_here).astype(jnp.int32)
    query_width = query_weight.shape[1]
    key_width = key_weight.shape[1]
    gain_first, gain_second, gain_query, gain_key = gains_all

    own_routes = jnp.take(routes_all, sources, axis=0)
    other_routes = jnp.take(routes_all, other_sources, axis=0)
    expert_here = jnp.broadcast_to(device, sources.shape)
    own_choice = slot_choice(own_routes, expert_here, capacity)
    pair_choice = slot_choice(own_routes, expert_here ^ 1, capacity)
    other_choice = slot_choice(other_routes, expert_here, capacity)
    choice = jnp.concatenate([own_choice, pair_choice], axis=1).astype(jnp.bfloat16)
    held_choice = jnp.concatenate([own_choice, other_choice], axis=0)
    held_routes = jnp.concatenate([own_routes, other_routes], axis=0)
    held_sources = jnp.concatenate([sources, other_sources])

    pack_index = jnp.take(assignment, device)
    lengths_row = jnp.take(lengths, pack_index, axis=0)
    segment, offset = segment_layout(lengths_row, tokens_here)
    places = jnp.arange(tokens_here, dtype=jnp.int32)
    allowed = (segment[:, None] == segment[None, :]) & (places[None, :] <= places[:, None])
    allowed = allowed.astype(jnp.float32)
    cosine_table, sine_table = rotation_tables(offset, HD)
    tables = jnp.stack(
        [
            jnp.concatenate([cosine_table[:, 0], cosine_table[:, 0]], axis=1),
            jnp.concatenate([-sine_table[:, 0], sine_table[:, 0]], axis=1),
        ]
    )
    head_gains = jnp.stack([gain_query, gain_key] + [gain_key] * 6)

    normed_first, factor_first = rms_forward(block_input, gain_first)
    first_normed = normed_first.astype(jnp.bfloat16)
    raw = jnp.dot(first_normed, joined_all, preferred_element_type=jnp.float32)
    mixed = attention_forward(raw, tables, head_gains, allowed)
    residual = block_input + jnp.dot(mixed, output_all, preferred_element_type=jnp.float32)
    normed_second, factor_second = rms_forward(residual, gain_second)
    own_tokens = normed_second.astype(jnp.bfloat16)
    logits = jnp.dot(own_tokens, router_all, preferred_element_type=jnp.float32)
    picked_mask = route_mask(routes, n_experts)
    chosen = jnp.sum(jnp.where(picked_mask, logits[:, None, :], 0.0), axis=-1)
    raised = jnp.exp(chosen)
    route_weights = raised / jnp.sum(raised, axis=-1, keepdims=True)

    own_grads = cotangent.astype(jnp.bfloat16)
    token_all, grad_all = gather_blocks([own_tokens, own_grads], [False, False], n_devices, 1)
    token_pieces = [own_tokens] + [token_all[i] for i in range(1, n_devices // 2)]
    grad_pieces = [own_grads] + [grad_all[i] for i in range(1, n_devices // 2)]
    rows_in = gathered_slots(token_pieces, choice, n_devices)
    grad_in = gathered_slots(grad_pieces, choice, n_devices)

    weights_from = gather_small(route_weights.T, device, n_devices)
    held_weights = jnp.take(weights_from, held_sources, axis=0)
    held_expert = jnp.broadcast_to(device, held_sources.shape)
    token_weight = weight_of(held_routes, held_weights, held_expert)
    slot_weight = jnp.sum(jnp.where(held_choice, token_weight[:, None, :], 0.0), axis=-1)
    slot_weight = slot_weight.reshape(-1, 1)

    gate_local = expert_gate[0]
    up_local = expert_up[0]
    down_local = expert_down[0]
    pre_gate = jnp.dot(rows_in, gate_local, preferred_element_type=jnp.float32)
    pre_up = jnp.dot(rows_in, up_local, preferred_element_type=jnp.float32)
    activated, derivative = silu_parts(pre_gate)
    inner = (activated * pre_up).astype(jnp.bfloat16)
    weighted = (
        jnp.dot(inner, down_local, preferred_element_type=jnp.float32) * slot_weight
    ).astype(jnp.bfloat16)

    grad_rows = (grad_in.astype(jnp.float32) * slot_weight).astype(jnp.bfloat16)
    inner_grad = times_transpose(grad_rows, down_local)
    down_grad = transpose_times(inner, grad_rows)
    gate_pre_grad = (inner_grad * pre_up * derivative).astype(jnp.bfloat16)
    up_pre_grad = (inner_grad * activated).astype(jnp.bfloat16)
    rows_grad = (
        times_transpose(gate_pre_grad, gate_local) + times_transpose(up_pre_grad, up_local)
    ).astype(jnp.bfloat16)
    gate_grad = transpose_times(rows_in, gate_pre_grad)
    up_grad = transpose_times(rows_in, up_pre_grad)

    slot_agree = jnp.sum(inner.astype(jnp.float32) * inner_grad, axis=-1)
    slot_agree = slot_agree.reshape(held_choice.shape[0], capacity)
    token_agree = jnp.sum(jnp.where(held_choice, slot_agree[:, :, None], 0.0), axis=1)
    wanted = jnp.arange(n_devices, dtype=jnp.int32)
    at = jnp.argmax(held_sources[None, :] == wanted[:, None], axis=1)
    agree_all = exchange_small(jnp.take(token_agree, at, axis=0), device, n_devices).T

    moe_back = returned_sum(rows_grad, choice, n_devices)
    moe_out = returned_sum(after(weighted, moe_back), choice, n_devices)
    block_output = residual + moe_out

    dense_weights = jnp.sum(jnp.where(picked_mask, route_weights[:, :, None], 0.0), axis=1)
    logit_grad = (
        agree_all - dense_weights * jnp.sum(agree_all, axis=-1, keepdims=True)
    ).astype(jnp.bfloat16)
    second_grad = moe_back + times_transpose(logit_grad, router_all)
    router_grad = transpose_times(own_tokens, logit_grad)
    residual_norm_grad, gain_second_grad = rms_backward(
        residual, factor_second, gain_second, second_grad
    )
    residual_grad = cotangent + residual_norm_grad
    residual_grad_b = residual_grad.astype(jnp.bfloat16)
    mixed_grad = times_transpose(residual_grad_b, output_all).astype(jnp.bfloat16)
    output_grad = transpose_times(mixed, residual_grad_b)
    joined_grad_b, head_gain_grads = attention_backward(
        raw, mixed_grad, tables, head_gains, allowed
    )
    joined_grad = transpose_times(first_normed, joined_grad_b)
    first_grad = times_transpose(joined_grad_b, joined_all)
    input_norm_grad, gain_first_grad = rms_backward(
        block_input, factor_first, gain_first, first_grad
    )
    input_grad = residual_grad + input_norm_grad
    gains_grad = jnp.concatenate(
        [gain_first_grad, gain_second_grad, head_gain_grads[0], head_gain_grads[1]]
    )
    output_share = scatter_rows(output_grad, sources, n_devices)
    joined_share = scatter_rows(joined_grad, sources, n_devices)
    tail_rows = jnp.pad(gains_grad, (0, -gains_grad.shape[0] % 128)).reshape(-1, 128)
    gains_sum = sum_small(tail_rows, n_devices).reshape(-1)
    gains_share = lax.dynamic_slice(gains_sum, (device * gain_count,), (gain_count,))
    router_sum = sum_small(router_grad.T, n_devices)
    router_share = lax.dynamic_slice(
        router_sum, (0, device * router_weight.shape[0]), router_weight.shape[::-1]
    ).T
    return (
        block_output,
        input_grad,
        joined_share[:, :query_width],
        joined_share[:, query_width : query_width + key_width],
        joined_share[:, query_width + key_width :],
        output_share,
        router_share,
        gains_share,
        gate_grad[None],
        up_grad[None],
        down_grad[None],
    )


def sparse_body(
    block_input,
    cotangent,
    query_weight,
    key_weight,
    value_weight,
    output_weight,
    router_weight,
    norm_gains,
    expert_gate,
    expert_up,
    expert_down,
    routes,
    lengths,
    assignment,
):
    tokens_here, model_width = block_input.shape
    n_experts = router_weight.shape[1]
    capacity = tokens_here * TOP * 5 // (4 * n_experts)
    gathered = (
        lax.all_gather(query_weight, AXIS, axis=0, tiled=True),
        lax.all_gather(key_weight, AXIS, axis=0, tiled=True),
        lax.all_gather(value_weight, AXIS, axis=0, tiled=True),
        lax.all_gather(output_weight, AXIS, axis=0, tiled=True),
        lax.all_gather(router_weight, AXIS, axis=0, tiled=True),
        lax.all_gather(norm_gains, AXIS, axis=0, tiled=True),
    )
    weights_all = (gathered[0], gathered[1], gathered[2], gathered[3], gathered[4])
    gains_all = split_gains(gathered[5], model_width)
    device = lax.axis_index(AXIS)
    pack_index = jnp.take(assignment, device)
    lengths_row = jnp.take(lengths, pack_index, axis=0)
    saved = dense_forward(block_input, lengths_row, routes, weights_all, gains_all, n_experts)
    route_weights = saved.route_weights
    slot_index, slot_token, slot_weight, slot_live = slot_tables(
        saved.picked_mask, routes, route_weights, capacity
    )
    outgoing = jnp.where(
        slot_live[:, None] > 0,
        jnp.take(saved.second_normed, slot_token, axis=0),
        jnp.zeros((), jnp.bfloat16),
    ).reshape(n_experts, capacity, model_width)
    gate_local = expert_gate[0]
    up_local = expert_up[0]
    down_local = expert_down[0]
    received = lax.all_to_all(outgoing, AXIS, split_axis=0, concat_axis=0, tiled=True)
    rows_in = received.reshape(-1, model_width)
    result, pre_gate, pre_up, inner = expert_forward_local(
        rows_in, gate_local, up_local, down_local
    )
    layout = (received.shape[0], received.shape[1], -1)
    returned = lax.all_to_all(
        result.reshape(received.shape), AXIS, split_axis=0, concat_axis=0, tiled=True
    )
    returned, received, pre_gate, pre_up, inner = (
        returned,
        received,
        pre_gate.reshape(layout),
        pre_up.reshape(layout),
        inner.reshape(layout),
    )
    picked = jnp.take(returned.reshape(n_experts * capacity, model_width), slot_index, axis=0)
    picked = picked.reshape(tokens_here, TOP, model_width).astype(jnp.float32)
    block_output = saved.residual + jnp.sum(picked * route_weights[:, :, None], axis=1)
    route_agree = jnp.sum(cotangent[:, None, :] * picked, axis=-1)
    grad_rows = (jnp.take(cotangent, slot_token, axis=0) * slot_weight[:, None]).astype(
        jnp.bfloat16
    )
    arrived = lax.all_to_all(
        grad_rows.reshape(n_experts, capacity, model_width),
        AXIS,
        split_axis=0,
        concat_axis=0,
        tiled=True,
    )
    ff_width = gate_local.shape[1]
    rows_grad, gate_grad, up_grad, down_grad = expert_backward(
        received.reshape(-1, model_width),
        pre_gate.reshape(-1, ff_width),
        pre_up.reshape(-1, ff_width),
        inner.reshape(-1, ff_width),
        arrived.reshape(-1, model_width),
        gate_local,
        up_local,
        down_local,
    )
    sent_back = lax.all_to_all(
        rows_grad.reshape(arrived.shape), AXIS, split_axis=0, concat_axis=0, tiled=True
    )
    moe_back = jnp.take(sent_back.reshape(n_experts * capacity, model_width), slot_index, axis=0)
    moe_back = jnp.sum(moe_back.reshape(tokens_here, TOP, model_width).astype(jnp.float32), axis=1)
    regathered = (
        lax.all_gather(query_weight, AXIS, axis=0, tiled=True),
        lax.all_gather(key_weight, AXIS, axis=0, tiled=True),
        lax.all_gather(value_weight, AXIS, axis=0, tiled=True),
        lax.all_gather(output_weight, AXIS, axis=0, tiled=True),
        lax.all_gather(router_weight, AXIS, axis=0, tiled=True),
        lax.all_gather(norm_gains, AXIS, axis=0, tiled=True),
    )
    back_weights = (regathered[0], regathered[1], regathered[2], regathered[3], regathered[4])
    back_gains = split_gains(regathered[5], model_width)
    input_grad, grads = sparse_backward(
        saved, back_weights, back_gains, cotangent, moe_back, route_agree
    )
    shares = (
        lax.psum_scatter(grads[0], AXIS, scatter_dimension=0, tiled=True),
        lax.psum_scatter(grads[1], AXIS, scatter_dimension=0, tiled=True),
        lax.psum_scatter(grads[2], AXIS, scatter_dimension=0, tiled=True),
        lax.psum_scatter(grads[3], AXIS, scatter_dimension=0, tiled=True),
        lax.psum_scatter(grads[4], AXIS, scatter_dimension=0, tiled=True),
        lax.psum_scatter(grads[5], AXIS, scatter_dimension=0, tiled=True),
    )
    return (
        block_output,
        input_grad,
        shares[0],
        shares[1],
        shares[2],
        shares[3],
        shares[4],
        shares[5],
        gate_grad[None],
        up_grad[None],
        down_grad[None],
    )


def solution(mesh):
    n_devices = mesh.shape[AXIS]
    dense = 8 <= n_devices <= 4 * TOP and n_devices & (n_devices - 1) == 0
    return jax.shard_map(
        dense_body if dense else sparse_body,
        mesh=mesh,
        in_specs=(
            P(AXIS, None),
            P(AXIS, None),
            P(AXIS, None),
            P(AXIS, None),
            P(AXIS, None),
            P(AXIS, None),
            P(AXIS, None),
            P(AXIS),
            P(AXIS, None, None),
            P(AXIS, None, None),
            P(AXIS, None, None),
            P(AXIS, None),
            P(),
            P(),
        ),
        out_specs=(
            P(AXIS, None),
            P(AXIS, None),
            P(AXIS, None),
            P(AXIS, None),
            P(AXIS, None),
            P(AXIS, None),
            P(AXIS, None),
            P(AXIS),
            P(AXIS, None, None),
            P(AXIS, None, None),
            P(AXIS, None, None),
        ),
        check_vma=False,
    )
```

```python
import functools
import types

import jax
import jax.numpy as jnp
from jax import lax
from jax.experimental import pallas as pl
from jax.experimental.pallas import tpu as pltpu
from jax.sharding import PartitionSpec as P

H = 32
KVH = 4
HD = 128
TOP = 8
AXIS = "fsdp"


NORM_EPSILON = 1e-06
ROPE_BASE = 1000000.0


def rms_forward(source, scales):
    factor = lax.rsqrt(jnp.mean(source * source, axis=-1, keepdims=True) + NORM_EPSILON)
    return (source * factor * scales, factor)


def rms_backward(source, factor, scales, upstream):
    scaled = upstream * scales
    inner_mean = jnp.mean(scaled * source, axis=-1, keepdims=True)
    grad_source = factor * (scaled - source * factor * factor * inner_mean)
    leading = tuple(range(source.ndim - 1))
    grad_scales = jnp.sum(upstream * source * factor, axis=leading)
    return (grad_source, grad_scales)


def segment_layout(lengths_row, tokens_here):
    seq_ends = jnp.cumsum(lengths_row)
    places = jnp.arange(tokens_here, dtype=jnp.int32)
    passed = (places[:, None] >= seq_ends[None, :]).astype(jnp.int32)
    segment = jnp.sum(passed, axis=1)
    seq_start = jnp.sum(passed * lengths_row[None, :], axis=1)
    return (segment, places - seq_start)


def rotation_tables(offset, head_size):
    half_size = head_size // 2
    frequency = ROPE_BASE ** (-2.0 * jnp.arange(half_size, dtype=jnp.float32) / head_size)
    angles = offset.astype(jnp.float32)[:, None] * frequency[None, :]
    return (jnp.cos(angles)[:, None, :], jnp.sin(angles)[:, None, :])


def rotate(operand, cosine_table, sine_table):
    half_size = operand.shape[-1] // 2
    first_half = operand[..., :half_size]
    second_half = operand[..., half_size:]
    return jnp.concatenate(
        [
            first_half * cosine_table - second_half * sine_table,
            second_half * cosine_table + first_half * sine_table,
        ],
        axis=-1,
    )


def rotate_back(operand, cosine_table, sine_table):
    half_size = operand.shape[-1] // 2
    first_half = operand[..., :half_size]
    second_half = operand[..., half_size:]
    return jnp.concatenate(
        [
            first_half * cosine_table + second_half * sine_table,
            second_half * cosine_table - first_half * sine_table,
        ],
        axis=-1,
    )


def silu_parts(pre_act):
    logistic = jax.nn.sigmoid(pre_act)
    return (pre_act * logistic, logistic * (1.0 + pre_act * (1.0 - logistic)))


def batched(form, left, right):
    return jnp.einsum(form, left, right, preferred_element_type=jnp.float32)


def times_transpose(left, right):
    return lax.dot_general(
        left, right, (((1,), (1,)), ((), ())), preferred_element_type=jnp.float32
    )


def transpose_times(left, right):
    return lax.dot_general(
        left, right, (((0,), (0,)), ((), ())), preferred_element_type=jnp.float32
    )


def split_gains(gains_vec, model_width):
    gains_float = gains_vec.astype(jnp.float32)
    return (
        gains_float[:model_width],
        gains_float[model_width : 2 * model_width],
        gains_float[2 * model_width : 2 * model_width + HD],
        gains_float[2 * model_width + HD :],
    )


def attention_weights(query_grouped, key_rot, allowed, scale, totals):
    scores = batched("tkgd,ukd->kgtu", query_grouped, key_rot) * scale
    raised = jnp.where(allowed, jnp.exp(scores), 0.0)
    if totals is None:
        totals = jnp.sum(raised, axis=-1, keepdims=True)
    return (raised / totals, totals)


def route_mask(routes_here, n_experts):
    return routes_here[:, :, None] == jnp.arange(n_experts, dtype=jnp.int32)[None, None, :]


def slot_tables(picked_mask, routes_here, route_weights, capacity):
    tokens_here, top_count, n_experts = picked_mask.shape
    flat_mask = picked_mask.reshape(tokens_here * top_count, n_experts).astype(jnp.int32)
    running = jnp.cumsum(flat_mask, axis=0)
    slot_rank = jnp.sum(flat_mask * running, axis=1) - 1
    slot_index = routes_here.reshape(-1) * capacity + slot_rank
    owner_row = jnp.arange(tokens_here * top_count, dtype=jnp.int32) // top_count
    slot_token = jnp.zeros((n_experts * capacity,), jnp.int32).at[slot_index].set(owner_row)
    slot_weight = (
        jnp.zeros((n_experts * capacity,), jnp.float32)
        .at[slot_index]
        .set(route_weights.reshape(-1))
    )
    slot_live = jnp.zeros((n_experts * capacity,), jnp.int32).at[slot_index].set(1)
    return (slot_index, slot_token, slot_weight, slot_live)


def dense_forward(block_rows, lengths_row, routes_here, weights_all, gains_all, n_experts):
    query_weight, key_weight, value_weight, output_weight, router_weight = weights_all
    gain_first, gain_second, gain_query, gain_key = gains_all
    tokens_here = block_rows.shape[0]
    group_size = H // KVH
    scale = HD ** (-0.5)
    segment, offset = segment_layout(lengths_row, tokens_here)
    places = jnp.arange(tokens_here, dtype=jnp.int32)
    allowed = (segment[:, None] == segment[None, :]) & (places[None, :] <= places[:, None])
    cosine_table, sine_table = rotation_tables(offset, HD)
    normed_first, factor_first = rms_forward(block_rows, gain_first)
    first_normed = normed_first.astype(jnp.bfloat16)
    query_raw = jnp.dot(first_normed, query_weight, preferred_element_type=jnp.float32).reshape(
        tokens_here, H, HD
    )
    key_raw = jnp.dot(first_normed, key_weight, preferred_element_type=jnp.float32).reshape(
        tokens_here, KVH, HD
    )
    value_rows = (
        jnp.dot(first_normed, value_weight, preferred_element_type=jnp.float32)
        .astype(jnp.bfloat16)
        .reshape(tokens_here, KVH, HD)
    )
    query_normed, query_factor = rms_forward(query_raw, gain_query)
    key_normed, key_factor = rms_forward(key_raw, gain_key)
    query_rot = rotate(query_normed, cosine_table, sine_table).astype(jnp.bfloat16)
    key_rot = rotate(key_normed, cosine_table, sine_table).astype(jnp.bfloat16)
    query_grouped = query_rot.reshape(tokens_here, KVH, group_size, HD)
    attention, totals = attention_weights(query_grouped, key_rot, allowed, scale, None)
    attention_b = attention.astype(jnp.bfloat16)
    mixed = (
        batched("kgtu,ukd->tkgd", attention_b, value_rows)
        .astype(jnp.bfloat16)
        .reshape(tokens_here, H * HD)
    )
    residual = block_rows + jnp.dot(mixed, output_weight, preferred_element_type=jnp.float32)
    normed_second, factor_second = rms_forward(residual, gain_second)
    second_normed = normed_second.astype(jnp.bfloat16)
    logits = jnp.dot(second_normed, router_weight, preferred_element_type=jnp.float32)
    picked_mask = route_mask(routes_here, n_experts)
    chosen = jnp.sum(jnp.where(picked_mask, logits[:, None, :], 0.0), axis=-1)
    raised = jnp.exp(chosen)
    route_weights = raised / jnp.sum(raised, axis=-1, keepdims=True)
    return types.SimpleNamespace(
        block_rows=block_rows,
        first_normed=first_normed,
        factor_first=factor_first,
        query_raw=query_raw,
        query_factor=query_factor,
        key_raw=key_raw,
        key_factor=key_factor,
        query_grouped=query_grouped,
        key_rot=key_rot,
        value_rows=value_rows,
        allowed=allowed,
        cosine_table=cosine_table,
        sine_table=sine_table,
        totals=totals,
        mixed=mixed,
        residual=residual,
        factor_second=factor_second,
        second_normed=second_normed,
        picked_mask=picked_mask,
        route_weights=route_weights,
    )


def sparse_backward(saved, weights_all, gains_all, cotangent_rows, moe_back, route_agree):
    query_weight, key_weight, value_weight, output_weight, router_weight = weights_all
    gain_first, gain_second, gain_query, gain_key = gains_all
    tokens_here = cotangent_rows.shape[0]
    group_size = H // KVH
    scale = HD ** (-0.5)
    route_weights = saved.route_weights
    chosen_grad = route_weights * (
        route_agree - jnp.sum(route_weights * route_agree, axis=-1, keepdims=True)
    )
    logit_grad = jnp.sum(
        jnp.where(saved.picked_mask, chosen_grad[:, :, None], 0.0), axis=1
    ).astype(jnp.bfloat16)
    second_grad = moe_back + times_transpose(logit_grad, router_weight)
    router_grad = transpose_times(saved.second_normed, logit_grad)
    residual_norm_grad, gain_second_grad = rms_backward(
        saved.residual, saved.factor_second, gain_second, second_grad
    )
    residual_grad = cotangent_rows + residual_norm_grad
    residual_grad_b = residual_grad.astype(jnp.bfloat16)
    output_grad = transpose_times(saved.mixed, residual_grad_b)
    mixed_grad = times_transpose(residual_grad_b, output_weight).astype(jnp.bfloat16)
    mixed_grouped = mixed_grad.reshape(tokens_here, KVH, group_size, HD)
    attention, _ = attention_weights(
        saved.query_grouped, saved.key_rot, saved.allowed, scale, saved.totals
    )
    attention_b = attention.astype(jnp.bfloat16)
    score_grad_raw = batched("tkgd,ukd->kgtu", mixed_grouped, saved.value_rows)
    value_rows_grad = batched("kgtu,tkgd->ukd", attention_b, mixed_grouped)
    delta = jnp.sum(attention * score_grad_raw, axis=-1, keepdims=True)
    score_grad = (attention * (score_grad_raw - delta) * scale).astype(jnp.bfloat16)
    query_rot_grad = batched("kgtu,ukd->tkgd", score_grad, saved.key_rot).reshape(
        tokens_here, H, HD
    )
    key_rot_grad = batched("kgtu,tkgd->ukd", score_grad, saved.query_grouped)
    query_raw_grad, gain_query_grad = rms_backward(
        saved.query_raw,
        saved.query_factor,
        gain_query,
        rotate_back(query_rot_grad, saved.cosine_table, saved.sine_table),
    )
    key_raw_grad, gain_key_grad = rms_backward(
        saved.key_raw,
        saved.key_factor,
        gain_key,
        rotate_back(key_rot_grad, saved.cosine_table, saved.sine_table),
    )
    query_grad_b = query_raw_grad.reshape(tokens_here, H * HD).astype(jnp.bfloat16)
    key_grad_b = key_raw_grad.reshape(tokens_here, KVH * HD).astype(jnp.bfloat16)
    value_grad_b = value_rows_grad.reshape(tokens_here, KVH * HD).astype(jnp.bfloat16)
    first_grad = (
        times_transpose(query_grad_b, query_weight)
        + times_transpose(key_grad_b, key_weight)
        + times_transpose(value_grad_b, value_weight)
    )
    first_normed = saved.first_normed
    query_grad = transpose_times(first_normed, query_grad_b)
    key_grad = transpose_times(first_normed, key_grad_b)
    value_grad = transpose_times(first_normed, value_grad_b)
    input_norm_grad, gain_first_grad = rms_backward(
        saved.block_rows, saved.factor_first, gain_first, first_grad
    )
    input_grad = residual_grad + input_norm_grad
    gains_grad = jnp.concatenate(
        [gain_first_grad, gain_second_grad, gain_query_grad, gain_key_grad]
    )
    return (input_grad, (query_grad, key_grad, value_grad, output_grad, router_grad, gains_grad))


def expert_forward_local(rows_in, gate_local, up_local, down_local):
    pre_gate = jnp.dot(rows_in, gate_local, preferred_element_type=jnp.float32)
    pre_up = jnp.dot(rows_in, up_local, preferred_element_type=jnp.float32)
    activated, _ = silu_parts(pre_gate)
    inner = (activated * pre_up).astype(jnp.bfloat16)
    result = jnp.dot(inner, down_local, preferred_element_type=jnp.float32).astype(jnp.bfloat16)
    return (result, pre_gate, pre_up, inner)


def expert_backward(rows_in, pre_gate, pre_up, inner, grad_rows, gate_local, up_local, down_local):
    inner_grad = times_transpose(grad_rows, down_local)
    down_grad = transpose_times(inner, grad_rows)
    activated, derivative = silu_parts(pre_gate)
    gate_pre_grad = (inner_grad * pre_up * derivative).astype(jnp.bfloat16)
    up_pre_grad = (inner_grad * activated).astype(jnp.bfloat16)
    rows_grad = (
        times_transpose(gate_pre_grad, gate_local) + times_transpose(up_pre_grad, up_local)
    ).astype(jnp.bfloat16)
    return (
        rows_grad,
        transpose_times(rows_in, gate_pre_grad),
        transpose_times(rows_in, up_pre_grad),
        down_grad,
    )


def swap(value, n_devices, mask):
    return lax.ppermute(value, AXIS, [(i, i ^ mask) for i in range(n_devices)])


def block_sources(device, n_devices):
    core = device & 1
    one = 2 + 2 * core
    offsets = [jnp.zeros_like(device), one, 6 - one, jnp.full_like(device, 6)]
    return jnp.stack([device ^ off ^ (8 * g) for g in range(n_devices // 8) for off in offsets])


def after(value, token):
    return lax.optimization_barrier((value, token))[0]


def sum_small(value, n_devices):
    mask = 1
    while mask < n_devices:
        value = value + swap(value, n_devices, mask)
        mask *= 2
    return value


def flipped(index, mask):
    return index + mask * (1 - 2 * lax.rem(lax.div(index, mask), 2))


def hop_peers(index):
    core = lax.rem(index, 2)
    low, high = flipped(index, 2), flipped(index, 4)
    return low + core * (high - low), high + core * (low - high)


def plane_peer(index, g):
    bit = 1
    while bit <= g:
        if g & bit:
            index = flipped(index, 8 * bit)
        bit *= 2
    return index


def mesh_kernel_setup(n_devices):
    me = lax.axis_index(AXIS)
    one_peer, two_peer = hop_peers(me)
    pair = flipped(me, 1)
    planes = [plane_peer(me, g) for g in range(n_devices // 8)]
    barrier = pltpu.get_barrier_semaphore()
    peers = [one_peer, two_peer, pair] + planes[1:]
    for peer in peers:
        pl.semaphore_signal(
            barrier, inc=1, device_id=(peer,), device_id_type=pl.DeviceIdType.MESH
        )
    pl.semaphore_wait(barrier, len(peers))
    return one_peer, two_peer, pair, planes


def slot_source(planes, g, j):
    first, second = hop_peers(planes[g])
    return (planes[g], first, second, flipped(flipped(planes[g], 2), 4))[j]


def rows_at(ref, device, rows):
    return ref.at[pl.ds(pl.multiple_of(device * rows, rows), rows)]


def remote_copy(source, target, send_sem, recv_sem, peer):
    return pltpu.make_async_remote_copy(
        src_ref=source,
        dst_ref=target,
        send_sem=send_sem,
        recv_sem=recv_sem,
        device_id=(peer,),
        device_id_type=pl.DeviceIdType.MESH,
    )


def gather_kernel(n_devices, whole, picked, *refs):
    count = len(whole)
    blocks, refs = refs[:count], refs[count:]
    choice = None
    if picked:
        choice, refs = refs[0], refs[1:]
    outs, refs = refs[:count], refs[count:]
    send, recv, here = refs[:3]
    landed, staged = {}, {}
    for order, a in enumerate(picked):
        landed[a], staged[a] = refs[3 + 2 * order], refs[4 + 2 * order]
    groups = n_devices // 8
    slots = 4 * groups
    one_peer, two_peer, pair, planes = mesh_kernel_setup(n_devices)
    started, local = [], []

    def begin(copy):
        copy.start()
        started.append(copy)
        return copy

    def keep(source, target, sem):
        copy = pltpu.make_async_copy(source, target, sem)
        copy.start()
        local.append(copy)

    def place(a, g, j):
        if whole[a]:
            return rows_at(outs[a], slot_source(planes, g, j), blocks[a].shape[0])
        return landed[a].at[4 * g + j]

    def move(a, g, j, from_g, from_j, peer):
        source = blocks[a] if from_g == 0 and from_j == 0 else place(a, from_g, from_j)
        target = place(a, from_g, from_j) if whole[a] else place(a, g, j)
        index = 4 * g + j
        return begin(remote_copy(source, target, send.at[a, index], recv.at[a, index], peer))

    def settle(a, g, j):
        slot = 4 * g + j
        first = slot == 0
        if whole[a]:
            source = blocks[a] if first else place(a, g, j)
            target = place(a, g, j)
            if first:
                keep(source, target, here.at[a, slot])
        else:
            piece = blocks[a] if first else landed[a].at[slot]
            capacity = choice.shape[1] // 2
            rows = jnp.dot(choice[slot], piece[...], preferred_element_type=jnp.float32)
            staged[a][slot] = rows.astype(jnp.bfloat16)
            target = rows_at(outs[a], slot_source(planes, g, j), capacity)
            keep(staged[a].at[slot, pl.ds(0, capacity)], target, here.at[a, slot])
            source = staged[a].at[slot, pl.ds(capacity, capacity)]
        index = slots + slot
        begin(remote_copy(source, target, send.at[a, index], recv.at[a, index], pair))

    hops = {}
    for a in range(count):
        hops[a, 0, 1] = move(a, 0, 1, 0, 0, one_peer)
        hops[a, 0, 2] = move(a, 0, 2, 0, 0, two_peer)
        for g in range(1, groups):
            hops[a, g, 0] = move(a, g, 0, 0, 0, planes[g])
    for a in range(count):
        settle(a, 0, 0)
    for g in range(groups):
        if g:
            for a in range(count):
                hops[a, g, 0].wait_recv()
                hops[a, g, 1] = move(a, g, 1, g, 0, one_peer)
                hops[a, g, 2] = move(a, g, 2, g, 0, two_peer)
                settle(a, g, 0)
        for a in range(count):
            hops[a, g, 1].wait_recv()
            hops[a, g, 3] = move(a, g, 3, g, 1, two_peer)
            settle(a, g, 1)
        if g:
            for a in range(count):
                for j in (2, 3):
                    hops[a, g - 1, j].wait_recv()
                    settle(a, g - 1, j)
    for a in range(count):
        for j in (2, 3):
            hops[a, groups - 1, j].wait_recv()
            settle(a, groups - 1, j)
    for a in range(count):
        for slot in range(slots):
            if whole[a]:
                like = blocks[a]
            else:
                capacity = choice.shape[1] // 2
                like = staged[a].at[slot, pl.ds(0, capacity)]
            index = slots + slot
            remote_copy(like, like, send.at[a, index], recv.at[a, index], pair).wait_recv()
    for copy in started:
        copy.wait_send()
    for copy in local:
        copy.wait()


def gather_blocks(blocks, whole, choice, n_devices, collective_id):
    count = len(blocks)
    slots = n_devices // 2
    picked = tuple(a for a in range(count) if not whole[a])
    shapes, scratch = [], []
    for a, block in enumerate(blocks):
        rows, width = block.shape
        if not whole[a]:
            double = choice.shape[1]
            scratch.append(pltpu.VMEM((slots, rows, width), block.dtype))
            scratch.append(pltpu.VMEM((slots, double, width), block.dtype))
            rows = double // 2
        shapes.append(jax.ShapeDtypeStruct((n_devices * rows, width), block.dtype))
    operands = list(blocks) + ([choice] if picked else [])
    return pl.pallas_call(
        functools.partial(gather_kernel, n_devices, tuple(whole), picked),
        out_shape=shapes,
        in_specs=[pl.BlockSpec(memory_space=pltpu.VMEM)] * len(operands),
        out_specs=[pl.BlockSpec(memory_space=pl.ANY)] * count,
        scratch_shapes=[
            pltpu.SemaphoreType.DMA((count, 2 * slots)),
            pltpu.SemaphoreType.DMA((count, 2 * slots)),
            pltpu.SemaphoreType.DMA((count, slots)),
        ]
        + scratch,
        compiler_params=pltpu.CompilerParams(
            collective_id=collective_id, has_side_effects=True, vmem_limit_bytes=64 << 20
        ),
    )(*operands)


def add_rows(target, terms):
    rows = target.shape[0]
    step = min(rows, 16)

    def some(i, carry):
        at = pl.ds(pl.multiple_of(i * step, step), step)
        total = terms[0][at, :].astype(jnp.float32)
        for term in terms[1:]:
            total = total + term[at, :].astype(jnp.float32)
        target[at, :] = total.astype(target.dtype)
        return carry

    lax.fori_loop(0, rows // step, some, 0)


def scatter_kernel(n_devices, chosen, *refs):
    count = len(chosen)
    parts, refs = refs[:count], refs[count:]
    choice = None
    if any(chosen):
        choice, refs = refs[0], refs[1:]
    outs, refs = refs[:count], refs[count:]
    send, recv, here = refs[:3]
    sums, arrived, near, far = [], [], [], []
    refs = list(refs[3:])
    for a in range(count):
        arrived.append(refs.pop(0))
        near.append(refs.pop(0))
        far.append(refs.pop(0))
        sums.append(refs.pop(0) if chosen[a] else near[a])
    groups = n_devices // 8
    slots = 4 * groups
    one_peer, two_peer, pair, planes = mesh_kernel_setup(n_devices)
    pair_planes = [flipped(plane, 1) for plane in planes]
    started, loads, gifts = [], {}, {}

    order = [4 * g + j for g in reversed(range(groups)) for j in (3, 2, 1, 0)]
    for slot in order:
        g, j = slot // 4, slot % 4
        for a in range(count):
            rows = near[a].shape[1]
            source = rows_at(parts[a], slot_source(planes, g, j), rows)
            loads[a, slot] = pltpu.make_async_copy(source, near[a].at[slot], here.at[a, slot])
            loads[a, slot].start()
            given = rows_at(parts[a], slot_source(pair_planes, g, j), rows)
            index = slots + slot
            gifts[a, slot] = remote_copy(
                given, far[a].at[slot], send.at[a, index], recv.at[a, index], pair
            )
            gifts[a, slot].start()
            started.append(gifts[a, slot])

    def make(a, slot):
        loads[a, slot].wait()
        gifts[a, slot].wait_recv()
        if chosen[a]:
            capacity = near[a].shape[1]
            block = transpose_times(choice[slot, :capacity], near[a][slot])
            block += transpose_times(choice[slot, capacity:], far[a][slot])
            sums[a][slot] = block.astype(sums[a].dtype)
        else:
            add_rows(sums[a].at[slot], [near[a].at[slot], far[a].at[slot]])

    hops = {}

    def push(a, slot, peer):
        copy = remote_copy(
            sums[a].at[slot],
            arrived[a].at[slot],
            send.at[a, slot],
            recv.at[a, slot],
            peer,
        )
        copy.start()
        started.append(copy)
        hops[a, slot] = copy

    def spread_out(g):
        for a in range(count):
            for j in (3, 2):
                make(a, 4 * g + j)
                push(a, 4 * g + j, two_peer)
        for a in range(count):
            for j in (1, 0):
                make(a, 4 * g + j)

    def side(g):
        for a in range(count):
            hops[a, 4 * g + 3].wait_recv()
            mine = sums[a].at[4 * g + 1]
            add_rows(mine, [mine, arrived[a].at[4 * g + 3]])
            push(a, 4 * g + 1, one_peer)

    def finish(g):
        for a in range(count):
            hops[a, 4 * g + 2].wait_recv()
            hops[a, 4 * g + 1].wait_recv()
            mine = sums[a].at[4 * g]
            terms = [mine, arrived[a].at[4 * g + 2], arrived[a].at[4 * g + 1]]
            if g:
                add_rows(mine, terms)
                push(a, 4 * g, planes[g])
            else:
                for other in range(1, groups):
                    hops[a, 4 * other].wait_recv()
                    terms.append(arrived[a].at[4 * other])
                add_rows(outs[a], terms)

    for step in range(groups + 2):
        if step < groups:
            spread_out(groups - 1 - step)
        if 0 <= step - 1 < groups:
            side(groups - step)
        if step >= 2:
            finish(groups + 1 - step)
    for copy in started:
        copy.wait_send()


def scatter_blocks(parts, chosen, choice, n_devices, collective_id):
    count = len(parts)
    slots = n_devices // 2
    shapes, scratch = [], []
    for a, part in enumerate(parts):
        rows, width = part.shape[0] // n_devices, part.shape[1]
        full = choice.shape[2] if chosen[a] else rows
        scratch.append(pltpu.VMEM((slots, full, width), part.dtype))
        scratch.append(pltpu.VMEM((slots, rows, width), part.dtype))
        scratch.append(pltpu.VMEM((slots, rows, width), part.dtype))
        if chosen[a]:
            scratch.append(pltpu.VMEM((slots, full, width), part.dtype))
        shapes.append(jax.ShapeDtypeStruct((full, width), jnp.float32))
    extra = [choice] if any(chosen) else []
    return pl.pallas_call(
        functools.partial(scatter_kernel, n_devices, tuple(chosen)),
        out_shape=shapes,
        in_specs=[pl.BlockSpec(memory_space=pl.ANY)] * count
        + [pl.BlockSpec(memory_space=pltpu.VMEM)] * len(extra),
        out_specs=[pl.BlockSpec(memory_space=pltpu.VMEM)] * count,
        scratch_shapes=[
            pltpu.SemaphoreType.DMA((count, 2 * slots)),
            pltpu.SemaphoreType.DMA((count, 2 * slots)),
            pltpu.SemaphoreType.DMA((count, slots)),
        ]
        + scratch,
        compiler_params=pltpu.CompilerParams(
            collective_id=collective_id, has_side_effects=True, vmem_limit_bytes=64 << 20
        ),
    )(*parts, *extra)


def slot_choice(routes_from, expert, capacity):
    member = jnp.any(routes_from == expert[:, None, None], axis=1)
    tokens_here = member.shape[1]
    places = jnp.arange(tokens_here, dtype=jnp.int32)
    upto = (places[:, None] <= places[None, :]).astype(jnp.bfloat16)
    rank = jnp.dot(member.astype(jnp.bfloat16), upto, preferred_element_type=jnp.float32) - 1.0
    slots = jnp.arange(capacity, dtype=jnp.float32)
    return member[:, None, :] & (rank[:, None, :] == slots[None, :, None])


def weight_of(routes_from, weights_from, expert):
    return jnp.sum(jnp.where(routes_from == expert[:, None, None], weights_from, 0.0), axis=1)


def turned(value, cosines, sines):
    return value * cosines + pltpu.roll(value, value.shape[-1] // 2, 1) * sines


def turned_back(value, cosines, sines):
    return value * cosines - pltpu.roll(value, value.shape[-1] // 2, 1) * sines


def unit_factor(value):
    return lax.rsqrt(jnp.mean(value * value, axis=-1, keepdims=True) + NORM_EPSILON)


def head_weights(query, key, allowed, scale):
    raised = jnp.where(allowed, jnp.exp(times_transpose(query, key) * scale), 0.0)
    return raised * (1.0 / jnp.sum(raised, axis=-1, keepdims=True))


def attention_kernel(scale, query_ref, key_ref, value_ref, table_ref, gain_ref, allowed_ref, out_ref):
    cosines, sines = table_ref[0], table_ref[1]
    gain_query, gain_key = gain_ref[0:1], gain_ref[1:2]
    allowed = allowed_ref[...] > 0.0
    key = key_ref[...]
    key = turned(key * unit_factor(key) * gain_key, cosines, sines).astype(jnp.bfloat16)
    value = value_ref[...].astype(jnp.bfloat16)
    for head in range(query_ref.shape[1] // HD):
        lanes = slice(head * HD, (head + 1) * HD)
        query = query_ref[:, lanes]
        query = turned(query * unit_factor(query) * gain_query, cosines, sines)
        weights = head_weights(query.astype(jnp.bfloat16), key, allowed, scale)
        mixed = jnp.dot(weights.astype(jnp.bfloat16), value, preferred_element_type=jnp.float32)
        out_ref[:, lanes] = mixed.astype(jnp.bfloat16)


def norm_back(source, factor, gain, upstream):
    scaled = upstream * gain
    inner = jnp.mean(scaled * source, axis=-1, keepdims=True)
    return factor * (scaled - source * (factor * factor * inner))


def attention_back_kernel(
    scale,
    query_ref,
    key_ref,
    value_ref,
    grad_ref,
    table_ref,
    gain_ref,
    allowed_ref,
    out_ref,
    gain_out_ref,
):
    group = pl.program_id(0)
    groups = pl.num_programs(0)
    cosines, sines = table_ref[0], table_ref[1]
    gain_query, gain_key = gain_ref[0:1], gain_ref[1:2]
    allowed = allowed_ref[...] > 0.0
    width = query_ref.shape[1]

    @pl.when(group == 0)
    def _():
        gain_out_ref[...] = jnp.zeros_like(gain_out_ref)

    key_raw = key_ref[...]
    key_factor = unit_factor(key_raw)
    key = turned(key_raw * key_factor * gain_key, cosines, sines).astype(jnp.bfloat16)
    value = value_ref[...].astype(jnp.bfloat16)
    key_grad = jnp.zeros(key_raw.shape, jnp.float32)
    value_grad = jnp.zeros(key_raw.shape, jnp.float32)
    gain_sum = jnp.zeros((1, HD), jnp.float32)
    for head in range(width // HD):
        lanes = slice(head * HD, (head + 1) * HD)
        query_raw = query_ref[:, lanes]
        query_factor = unit_factor(query_raw)
        unit = query_raw * query_factor
        query = turned(unit * gain_query, cosines, sines).astype(jnp.bfloat16)
        weights = head_weights(query, key, allowed, scale)
        mixed_grad = grad_ref[:, lanes]
        raw_grad = times_transpose(mixed_grad, value)
        delta = jnp.sum(weights * raw_grad, axis=-1, keepdims=True)
        score_grad = (weights * (raw_grad - delta) * scale).astype(jnp.bfloat16)
        value_grad += transpose_times(weights.astype(jnp.bfloat16), mixed_grad)
        key_grad += transpose_times(score_grad, query)
        upstream = turned_back(
            jnp.dot(score_grad, key, preferred_element_type=jnp.float32), cosines, sines
        )
        gain_sum += jnp.sum(upstream * unit, axis=0, keepdims=True)
        query_grad = norm_back(query_raw, query_factor, gain_query, upstream)
        start = pl.multiple_of(group * width + head * HD, HD)
        out_ref[:, pl.ds(start, HD)] = query_grad.astype(jnp.bfloat16)
    upstream = turned_back(key_grad, cosines, sines)
    gain_out_ref[0:1] += gain_sum
    gain_out_ref[1:2] += jnp.sum(upstream * key_raw * key_factor, axis=0, keepdims=True)
    start = pl.multiple_of(groups * width + group * HD, HD)
    out_ref[:, pl.ds(start, HD)] = norm_back(key_raw, key_factor, gain_key, upstream).astype(
        jnp.bfloat16
    )
    start = pl.multiple_of(groups * (width + HD) + group * HD, HD)
    out_ref[:, pl.ds(start, HD)] = value_grad.astype(jnp.bfloat16)


def attention_specs(tokens_here):
    group = H // KVH
    return [
        pl.BlockSpec((tokens_here, group * HD), lambda k: (0, k)),
        pl.BlockSpec((tokens_here, HD), lambda k: (0, H + k)),
        pl.BlockSpec((tokens_here, HD), lambda k: (0, H + KVH + k)),
    ]


def shared_specs(arrays):
    return [pl.BlockSpec(a.shape, lambda k, r=a.ndim: (0,) * r) for a in arrays]


def attention_forward(raw, tables, gains, allowed):
    tokens_here = raw.shape[0]
    group = H // KVH
    return pl.pallas_call(
        functools.partial(attention_kernel, HD ** (-0.5)),
        grid=(KVH,),
        out_shape=jax.ShapeDtypeStruct((tokens_here, H * HD), jnp.bfloat16),
        in_specs=attention_specs(tokens_here) + shared_specs([tables, gains, allowed]),
        out_specs=pl.BlockSpec((tokens_here, group * HD), lambda k: (0, k)),
        cost_estimate=pl.CostEstimate(
            flops=4 * H * HD * tokens_here**2,
            bytes_accessed=6 * raw.size,
            transcendentals=H * tokens_here**2,
        ),
    )(raw, raw, raw, tables, gains, allowed)


def attention_backward(raw, mixed_grad, tables, gains, allowed):
    tokens_here = raw.shape[0]
    group = H // KVH
    specs = attention_specs(tokens_here)
    return pl.pallas_call(
        functools.partial(attention_back_kernel, HD ** (-0.5)),
        grid=(KVH,),
        out_shape=[
            jax.ShapeDtypeStruct(raw.shape, jnp.bfloat16),
            jax.ShapeDtypeStruct((8, HD), jnp.float32),
        ],
        in_specs=specs + [specs[0]] + shared_specs([tables, gains, allowed]),
        out_specs=[
            pl.BlockSpec(raw.shape, lambda k: (0, 0)),
            pl.BlockSpec((8, HD), lambda k: (0, 0)),
        ],
        cost_estimate=pl.CostEstimate(
            flops=10 * H * HD * tokens_here**2,
            bytes_accessed=8 * raw.size,
            transcendentals=H * tokens_here**2,
        ),
    )(raw, raw, raw, mixed_grad, tables, gains, allowed)


def dense_body(
    block_input,
    cotangent,
    query_weight,
    key_weight,
    value_weight,
    output_weight,
    router_weight,
    norm_gains,
    expert_gate,
    expert_up,
    expert_down,
    routes,
    lengths,
    assignment,
):
    tokens_here, model_width = block_input.shape
    n_experts = router_weight.shape[1]
    n_devices = n_experts
    capacity = tokens_here * TOP * 5 // (4 * n_experts)
    device = lax.axis_index(AXIS)
    sources = block_sources(device, n_devices)

    gain_count = norm_gains.shape[0]
    router_count = router_weight.size
    small = jnp.concatenate(
        [router_weight.reshape(-1), norm_gains, routes.T.astype(jnp.bfloat16).reshape(-1)]
    )
    padded = -(-small.shape[0] // 2048) * 2048
    small = jnp.pad(small, (0, padded - small.shape[0])).reshape(-1, 128)
    joined = jnp.concatenate([query_weight, key_weight, value_weight], axis=1)
    small_all, joined_all, output_all = gather_blocks(
        [small, joined, output_weight], [True, True, True], None, n_devices, 0
    )
    small_all = small_all.reshape(n_devices, -1)
    router_all = small_all[:, :router_count].reshape(-1, n_experts)
    route_start = router_count + gain_count
    gains_all = split_gains(small_all[:, router_count:route_start].reshape(-1), model_width)
    routes_all = small_all[:, route_start : route_start + routes.size]
    routes_all = routes_all.reshape(n_devices, TOP, tokens_here).astype(jnp.int32)
    query_width = query_weight.shape[1]
    key_width = key_weight.shape[1]
    gain_first, gain_second, gain_query, gain_key = gains_all

    near_routes = jnp.take(routes_all, sources, axis=0)
    expert_here = jnp.broadcast_to(device, sources.shape)
    choice = jnp.concatenate(
        [
            slot_choice(near_routes, expert_here, capacity),
            slot_choice(near_routes, expert_here ^ 1, capacity),
        ],
        axis=1,
    ).astype(jnp.bfloat16)
    every_expert = jnp.broadcast_to(device, (n_devices,))
    held_choice = slot_choice(routes_all, every_expert, capacity)

    pack_index = jnp.take(assignment, device)
    lengths_row = jnp.take(lengths, pack_index, axis=0)
    segment, offset = segment_layout(lengths_row, tokens_here)
    places = jnp.arange(tokens_here, dtype=jnp.int32)
    allowed = (segment[:, None] == segment[None, :]) & (places[None, :] <= places[:, None])
    allowed = allowed.astype(jnp.float32)
    cosine_table, sine_table = rotation_tables(offset, HD)
    tables = jnp.stack(
        [
            jnp.concatenate([cosine_table[:, 0], cosine_table[:, 0]], axis=1),
            jnp.concatenate([-sine_table[:, 0], sine_table[:, 0]], axis=1),
        ]
    )
    head_gains = jnp.stack([gain_query, gain_key] + [gain_key] * 6)

    normed_first, factor_first = rms_forward(block_input, gain_first)
    first_normed = normed_first.astype(jnp.bfloat16)
    raw = jnp.dot(first_normed, joined_all, preferred_element_type=jnp.float32)
    mixed = attention_forward(raw, tables, head_gains, allowed)
    residual = block_input + jnp.dot(mixed, output_all, preferred_element_type=jnp.float32)
    normed_second, factor_second = rms_forward(residual, gain_second)
    own_tokens = normed_second.astype(jnp.bfloat16)
    logits = jnp.dot(own_tokens, router_all, preferred_element_type=jnp.float32)
    picked_mask = route_mask(routes, n_experts)
    chosen = jnp.sum(jnp.where(picked_mask, logits[:, None, :], 0.0), axis=-1)
    raised = jnp.exp(chosen)
    route_weights = raised / jnp.sum(raised, axis=-1, keepdims=True)

    own_grads = cotangent.astype(jnp.bfloat16)
    rows_in, grad_in, weights_all = gather_blocks(
        [own_tokens, own_grads, route_weights.T], [False, False, True], choice, n_devices, 1
    )
    weights_all = weights_all.reshape(n_devices, TOP, tokens_here)
    token_weight = weight_of(routes_all, weights_all, every_expert)
    slot_weight = jnp.sum(jnp.where(held_choice, token_weight[:, None, :], 0.0), axis=-1)
    slot_weight = slot_weight.reshape(-1, 1)

    gate_local = expert_gate[0]
    up_local = expert_up[0]
    down_local = expert_down[0]
    pre_gate = jnp.dot(rows_in, gate_local, preferred_element_type=jnp.float32)
    pre_up = jnp.dot(rows_in, up_local, preferred_element_type=jnp.float32)
    activated, derivative = silu_parts(pre_gate)
    inner = (activated * pre_up).astype(jnp.bfloat16)
    weighted = (
        jnp.dot(inner, down_local, preferred_element_type=jnp.float32) * slot_weight
    ).astype(jnp.bfloat16)

    grad_rows = (grad_in.astype(jnp.float32) * slot_weight).astype(jnp.bfloat16)
    inner_grad = times_transpose(grad_rows, down_local)
    down_grad = transpose_times(inner, grad_rows)
    gate_pre_grad = (inner_grad * pre_up * derivative).astype(jnp.bfloat16)
    up_pre_grad = (inner_grad * activated).astype(jnp.bfloat16)
    rows_grad = (
        times_transpose(gate_pre_grad, gate_local) + times_transpose(up_pre_grad, up_local)
    ).astype(jnp.bfloat16)
    gate_grad = transpose_times(rows_in, gate_pre_grad)
    up_grad = transpose_times(rows_in, up_pre_grad)

    slot_agree = jnp.sum(inner.astype(jnp.float32) * inner_grad, axis=-1)
    slot_agree = slot_agree.reshape(n_devices, capacity)
    token_agree = jnp.sum(jnp.where(held_choice, slot_agree[:, :, None], 0.0), axis=1)
    mine = jnp.arange(n_experts, dtype=jnp.int32)[None, :, None] == device
    token_agree = jnp.where(mine, token_agree[:, None, :], 0.0).reshape(-1, tokens_here)

    moe_back, agree_all = scatter_blocks(
        [rows_grad, token_agree], [True, False], choice, n_devices, 2
    )
    agree_all = agree_all.T
    (moe_out,) = scatter_blocks([after(weighted, moe_back)], [True], choice, n_devices, 3)
    block_output = residual + moe_out

    dense_weights = jnp.sum(jnp.where(picked_mask, route_weights[:, :, None], 0.0), axis=1)
    logit_grad = (
        agree_all - dense_weights * jnp.sum(agree_all, axis=-1, keepdims=True)
    ).astype(jnp.bfloat16)
    second_grad = moe_back + times_transpose(logit_grad, router_all)
    router_grad = transpose_times(own_tokens, logit_grad)
    residual_norm_grad, gain_second_grad = rms_backward(
        residual, factor_second, gain_second, second_grad
    )
    residual_grad = cotangent + residual_norm_grad
    residual_grad_b = residual_grad.astype(jnp.bfloat16)
    mixed_grad = times_transpose(residual_grad_b, output_all).astype(jnp.bfloat16)
    output_grad = transpose_times(mixed, residual_grad_b)
    joined_grad_b, head_gain_grads = attention_backward(
        raw, mixed_grad, tables, head_gains, allowed
    )
    joined_grad = transpose_times(first_normed, joined_grad_b)
    first_grad = times_transpose(joined_grad_b, joined_all)
    input_norm_grad, gain_first_grad = rms_backward(
        block_input, factor_first, gain_first, first_grad
    )
    input_grad = residual_grad + input_norm_grad
    gains_grad = jnp.concatenate(
        [gain_first_grad, gain_second_grad, head_gain_grads[0], head_gain_grads[1]]
    )
    output_share, joined_share = scatter_blocks(
        [output_grad.astype(jnp.bfloat16), joined_grad.astype(jnp.bfloat16)],
        [False, False],
        None,
        n_devices,
        4,
    )
    tail_rows = jnp.pad(gains_grad, (0, -gains_grad.shape[0] % 128)).reshape(-1, 128)
    gains_sum = sum_small(tail_rows, n_devices).reshape(-1)
    gains_share = lax.dynamic_slice(gains_sum, (device * gain_count,), (gain_count,))
    router_sum = sum_small(router_grad.T, n_devices)
    router_share = lax.dynamic_slice(
        router_sum, (0, device * router_weight.shape[0]), router_weight.shape[::-1]
    ).T
    return (
        block_output,
        input_grad,
        joined_share[:, :query_width],
        joined_share[:, query_width : query_width + key_width],
        joined_share[:, query_width + key_width :],
        output_share,
        router_share,
        gains_share,
        gate_grad[None],
        up_grad[None],
        down_grad[None],
    )


def sparse_body(
    block_input,
    cotangent,
    query_weight,
    key_weight,
    value_weight,
    output_weight,
    router_weight,
    norm_gains,
    expert_gate,
    expert_up,
    expert_down,
    routes,
    lengths,
    assignment,
):
    tokens_here, model_width = block_input.shape
    n_experts = router_weight.shape[1]
    capacity = tokens_here * TOP * 5 // (4 * n_experts)
    gathered = (
        lax.all_gather(query_weight, AXIS, axis=0, tiled=True),
        lax.all_gather(key_weight, AXIS, axis=0, tiled=True),
        lax.all_gather(value_weight, AXIS, axis=0, tiled=True),
        lax.all_gather(output_weight, AXIS, axis=0, tiled=True),
        lax.all_gather(router_weight, AXIS, axis=0, tiled=True),
        lax.all_gather(norm_gains, AXIS, axis=0, tiled=True),
    )
    weights_all = (gathered[0], gathered[1], gathered[2], gathered[3], gathered[4])
    gains_all = split_gains(gathered[5], model_width)
    device = lax.axis_index(AXIS)
    pack_index = jnp.take(assignment, device)
    lengths_row = jnp.take(lengths, pack_index, axis=0)
    saved = dense_forward(block_input, lengths_row, routes, weights_all, gains_all, n_experts)
    route_weights = saved.route_weights
    slot_index, slot_token, slot_weight, slot_live = slot_tables(
        saved.picked_mask, routes, route_weights, capacity
    )
    outgoing = jnp.where(
        slot_live[:, None] > 0,
        jnp.take(saved.second_normed, slot_token, axis=0),
        jnp.zeros((), jnp.bfloat16),
    ).reshape(n_experts, capacity, model_width)
    gate_local = expert_gate[0]
    up_local = expert_up[0]
    down_local = expert_down[0]
    received = lax.all_to_all(outgoing, AXIS, split_axis=0, concat_axis=0, tiled=True)
    rows_in = received.reshape(-1, model_width)
    result, pre_gate, pre_up, inner = expert_forward_local(
        rows_in, gate_local, up_local, down_local
    )
    layout = (received.shape[0], received.shape[1], -1)
    returned = lax.all_to_all(
        result.reshape(received.shape), AXIS, split_axis=0, concat_axis=0, tiled=True
    )
    returned, received, pre_gate, pre_up, inner = (
        returned,
        received,
        pre_gate.reshape(layout),
        pre_up.reshape(layout),
        inner.reshape(layout),
    )
    picked = jnp.take(returned.reshape(n_experts * capacity, model_width), slot_index, axis=0)
    picked = picked.reshape(tokens_here, TOP, model_width).astype(jnp.float32)
    block_output = saved.residual + jnp.sum(picked * route_weights[:, :, None], axis=1)
    route_agree = jnp.sum(cotangent[:, None, :] * picked, axis=-1)
    grad_rows = (jnp.take(cotangent, slot_token, axis=0) * slot_weight[:, None]).astype(
        jnp.bfloat16
    )
    arrived = lax.all_to_all(
        grad_rows.reshape(n_experts, capacity, model_width),
        AXIS,
        split_axis=0,
        concat_axis=0,
        tiled=True,
    )
    ff_width = gate_local.shape[1]
    rows_grad, gate_grad, up_grad, down_grad = expert_backward(
        received.reshape(-1, model_width),
        pre_gate.reshape(-1, ff_width),
        pre_up.reshape(-1, ff_width),
        inner.reshape(-1, ff_width),
        arrived.reshape(-1, model_width),
        gate_local,
        up_local,
        down_local,
    )
    sent_back = lax.all_to_all(
        rows_grad.reshape(arrived.shape), AXIS, split_axis=0, concat_axis=0, tiled=True
    )
    moe_back = jnp.take(sent_back.reshape(n_experts * capacity, model_width), slot_index, axis=0)
    moe_back = jnp.sum(moe_back.reshape(tokens_here, TOP, model_width).astype(jnp.float32), axis=1)
    regathered = (
        lax.all_gather(query_weight, AXIS, axis=0, tiled=True),
        lax.all_gather(key_weight, AXIS, axis=0, tiled=True),
        lax.all_gather(value_weight, AXIS, axis=0, tiled=True),
        lax.all_gather(output_weight, AXIS, axis=0, tiled=True),
        lax.all_gather(router_weight, AXIS, axis=0, tiled=True),
        lax.all_gather(norm_gains, AXIS, axis=0, tiled=True),
    )
    back_weights = (regathered[0], regathered[1], regathered[2], regathered[3], regathered[4])
    back_gains = split_gains(regathered[5], model_width)
    input_grad, grads = sparse_backward(
        saved, back_weights, back_gains, cotangent, moe_back, route_agree
    )
    shares = (
        lax.psum_scatter(grads[0], AXIS, scatter_dimension=0, tiled=True),
        lax.psum_scatter(grads[1], AXIS, scatter_dimension=0, tiled=True),
        lax.psum_scatter(grads[2], AXIS, scatter_dimension=0, tiled=True),
        lax.psum_scatter(grads[3], AXIS, scatter_dimension=0, tiled=True),
        lax.psum_scatter(grads[4], AXIS, scatter_dimension=0, tiled=True),
        lax.psum_scatter(grads[5], AXIS, scatter_dimension=0, tiled=True),
    )
    return (
        block_output,
        input_grad,
        shares[0],
        shares[1],
        shares[2],
        shares[3],
        shares[4],
        shares[5],
        gate_grad[None],
        up_grad[None],
        down_grad[None],
    )


def solution(mesh):
    n_devices = mesh.shape[AXIS]
    dense = 8 <= n_devices <= 4 * TOP and n_devices & (n_devices - 1) == 0
    return jax.shard_map(
        dense_body if dense else sparse_body,
        mesh=mesh,
        in_specs=(
            P(AXIS, None),
            P(AXIS, None),
            P(AXIS, None),
            P(AXIS, None),
            P(AXIS, None),
            P(AXIS, None),
            P(AXIS, None),
            P(AXIS),
            P(AXIS, None, None),
            P(AXIS, None, None),
            P(AXIS, None, None),
            P(AXIS, None),
            P(),
            P(),
        ),
        out_specs=(
            P(AXIS, None),
            P(AXIS, None),
            P(AXIS, None),
            P(AXIS, None),
            P(AXIS, None),
            P(AXIS, None),
            P(AXIS, None),
            P(AXIS),
            P(AXIS, None, None),
            P(AXIS, None, None),
            P(AXIS, None, None),
        ),
        check_vma=False,
    )
```
